256 devices in a mesh: dp: 8 (over y, core), seq: 32 (over x, z).
Axes of the slice: x: 4, y: 4, z: 8, core: 2. Of those that a mesh axis runs over, the one named last changes fastest.
Arguments:
- means: bfloat16 [2048, 384, 192], P('dp', 'seq'), may hold values from -6 to 6
- log_scales: bfloat16 [2048, 384, 192], P('dp', 'seq'), may hold values from -0.5 to 0.5
- latents: bfloat16 [2048, 1536, 192], P('dp', 'seq'), may hold values from -7 to 7
- text_lens: int32 [2048], P('dp'), may hold values from 96 to 384
- frame_lens: int32 [2048], P('dp'), may hold values from 384 to 1536
Outputs:
- positions: float32 [2048, 1536], P('dp', 'seq')
- loss: float32 [], replicated
The draws below stay inside these ranges and needn't reach their ends.
Inputs may be any that keep to these rules, and one draw needn't show every extreme that they name: `frame_lens`: each utterance has at least as many frames as any text can have tokens.
All inputs are finite; a program needn't handle non-finite values.
Results may differ from the reference program's by a relative error of at most 0.0065.
Values may be sent and summed in bfloat16 or wider, within the bound.
No kernel may reach another device: no remote copies, remote signals or barrier semaphores. Data moves between devices by JAX's collectives and lax.ppermute only.
A program may use at most 128 MiB of HBM per device.

```python
import math
import jax
import jax.numpy as jnp
from jax import lax

C = 192
TXT = 384
FR = 1536
UTT = 2048


def set_ends(drawn, stream_key, smallest, top_value):
    extent = drawn.shape
    index_at = [jax.random.randint(jax.random.fold_in(stream_key, axis), (), 0, extent[axis]) for axis in range(len(extent))]
    drawn = drawn.at[tuple(index_at)].set(smallest)
    longest = extent.index(max(extent))
    index_at[longest] = (index_at[longest] + 1) % extent[longest]
    return drawn.at[tuple(index_at)].set(top_value)


def shard_levels(rng, shape, cuts, low, high):
    def one(axis_at, blocks):
        draws = jax.random.uniform(jax.random.fold_in(jax.random.fold_in(rng, 6), axis_at), (blocks,), jnp.float32, low / len(cuts), high / len(cuts))
        return jnp.repeat(jnp.exp(draws), shape[axis_at] // blocks).reshape((-1,) + (1,) * (len(shape) - axis_at - 1))

    loudness = one(*cuts[0])
    for cut in cuts[1:]:
        loudness = loudness * one(*cut)
    return loudness


def normal_values(stream_key, shape, scale, most, split=(), held_as=jnp.bfloat16):
    entries = scale * jax.random.normal(stream_key, shape, jnp.float32)
    if split:
        entries = entries * shard_levels(stream_key, shape, split, -0.22, 0.18)
    return jnp.clip(entries, -most, most).astype(held_as)


def setup_inputs(seed: int = 0) -> dict:
    keys = jax.random.split(jax.random.key(seed), 6)
    means = normal_values(keys[0], (UTT, TXT, C), 1.0, 6.0, ((0, 8), (1, 32)))
    log_scales = jnp.clip(jax.random.uniform(keys[1], (UTT, TXT, C), jnp.float32, -0.5, 0.5) * shard_levels(keys[1], (UTT, TXT, C), ((0, 8), (1, 32)), -0.4, 0.0), -0.5, 0.5).astype(jnp.bfloat16)
    latents = normal_values(keys[2], (UTT, FR, C), 1.2, 7.0, ((0, 8), (1, 32)))
    text_lens = set_ends(jax.random.randint(keys[3], (UTT,), TXT // 4, TXT + 1), jax.random.fold_in(keys[3], 1), TXT // 4, TXT).astype(jnp.int32)
    frame_lens = set_ends(jax.random.randint(keys[4], (UTT,), TXT, FR + 1), jax.random.fold_in(keys[4], 1), TXT, FR).astype(jnp.int32)
    return {"means": means, "log_scales": log_scales, "latents": latents, "text_lens": text_lens, "frame_lens": frame_lens}


HALF_LOG_TWO_PI = 0.9189385332046727
NEG_FILL = -1.0e9


def prior_terms(means, log_scales):
    mean_wide = means.astype(jnp.float32)
    scale_wide = log_scales.astype(jnp.float32)
    precision = jnp.exp(-2.0 * scale_wide)
    weighted = (mean_wide * precision).astype(jnp.bfloat16)
    prec_low = precision.astype(jnp.bfloat16)
    channels = means.shape[-1]
    offset = (0.5 * jnp.sum(mean_wide * mean_wide * precision, axis=-1) + jnp.sum(scale_wide, axis=-1)) / channels + HALF_LOG_TWO_PI
    return weighted, prec_low, offset


def frame_update(previous, loglik, frame_id, text_len, frame_len, token_ids):
    batch = previous.shape[0]
    shifted = jnp.concatenate([jnp.full((batch, 1), NEG_FILL, previous.dtype), previous[:, :-1]], axis=1)
    lower = text_len[:, None] - frame_len[:, None] + frame_id
    allowed = (token_ids[None, :] < text_len[:, None]) & (frame_id < frame_len[:, None]) & (token_ids[None, :] <= frame_id) & (token_ids[None, :] >= lower)
    scores = jnp.where(allowed, loglik + jnp.maximum(previous, shifted), NEG_FILL)
    summit = jnp.max(scores, axis=1, keepdims=True)
    weight = jnp.exp(scores - summit)
    centre = jnp.sum(weight * token_ids.astype(scores.dtype)[None, :], axis=1) / jnp.sum(weight, axis=1)
    position = jnp.where(frame_id < frame_len, centre / (text_len - 1).astype(scores.dtype), 0.0)
    closing_value = (token_ids[None, :] == text_len[:, None] - 1) & (frame_id == frame_len[:, None] - 1)
    gained = jnp.sum(jnp.where(closing_value, scores, 0.0), axis=1)
    return scores, position, gained


def reference(means, log_scales, latents, text_lens, frame_lens):
    utter_all = means.shape[0]
    group = math.gcd(utter_all, 64)
    groups = utter_all // group
    weighted, prec_low, offset = prior_terms(means, log_scales)
    token_ids = jnp.arange(TXT, dtype=jnp.int32)
    frame_ids = jnp.arange(FR, dtype=jnp.int32)

    def one_group(inputs):
        latent_group, weighted_latent_group, precision_group, offset_group, text_group, frame_group = inputs
        latent_broadened = latent_group.astype(jnp.float32)
        squared_latent = lax.optimization_barrier((latent_broadened * latent_broadened).astype(jnp.bfloat16)).astype(jnp.float32)
        cross_product_term = jnp.einsum("zne,zje->znj", latent_broadened, weighted_latent_group.astype(jnp.float32))
        quadratic_term = jnp.einsum("zne,zje->znj", squared_latent, precision_group.astype(jnp.float32))
        loglik = (cross_product_term - 0.5 * quadratic_term) / C - offset_group[:, None, :]
        initial = jnp.broadcast_to(jnp.where(token_ids == 0, 0.0, NEG_FILL).astype(jnp.float32), (group, TXT))

        def step(carried, inputs_now):
            previous, finish = carried
            frame_like, frame_id = inputs_now
            scores, position, gained = frame_update(previous, frame_like, frame_id, text_group, frame_group, token_ids)
            return (scores, finish + gained), position

        carried, positions = lax.scan(step, (initial, jnp.zeros((group,), jnp.float32)), (jnp.moveaxis(loglik, 1, 0), frame_ids))
        return jnp.moveaxis(positions, 0, 1), carried[1]

    inputs = (latents.reshape(groups, group, FR, C), weighted.reshape(groups, group, TXT, C), prec_low.reshape(groups, group, TXT, C), offset.reshape(groups, group, TXT), text_lens.reshape(groups, group), frame_lens.reshape(groups, group))
    positions, finish = lax.map(one_group, inputs)
    loss = -jnp.sum(finish) / jnp.sum(frame_lens).astype(jnp.float32)
    return positions.reshape(utter_all, FR), loss
```

```python
import functools
import math

import jax
import jax.numpy as jnp
from jax import lax
from jax.experimental import pallas as pl
from jax.experimental.pallas import tpu as pltpu
from jax.sharding import Mesh
from jax.sharding import PartitionSpec as P

SEQ = ("seq_0", "seq_1")
DP = ("dp_0", "dp_1")

C = 192
TXT = 384
FR = 1536
OWN = 32
GRP = 256
TB = TXT // OWN
FB = FR // OWN
NU = 4
NCH = GRP // OWN // NU
ROWS = (NU + NU // 2) * FB
PROWS = (GRP // OWN) * 3 // 2 * TB
PAD = 296
NK = 2 * (NU + NU // 2) * 128
NN = TB * 128
MB = 384

HALF_LOG_TWO_PI = 0.9189385332046727
NEG = -2.0e11
F32 = jnp.float32
BF16 = jnp.bfloat16
NT = (((1,), (1,)), ((), ()))
NN_DIMS = (((1,), (0,)), ((), ()))


def params():
    return pltpu.CompilerParams(vmem_limit_bytes=60 * 1024 * 1024)


def call(body, out_shape, n_in, scratch=(), smem=()):
    vmem = pl.BlockSpec(memory_space=pltpu.VMEM)
    return pl.pallas_call(
        body,
        out_shape=out_shape,
        in_specs=[pl.BlockSpec(memory_space=pltpu.SMEM) if i in smem else vmem for i in range(n_in)],
        out_specs=jax.tree.map(lambda _: vmem, out_shape),
        scratch_shapes=list(scratch),
        compiler_params=params(),
    )


def one_hot(rank_row, first, count, dtype):
    ids = lax.broadcasted_iota(jnp.int32, (count, GRP), 0) + first
    return jnp.where(ids == rank_row, 1.0, 0.0).astype(dtype)


def pack_block(x, picks, stage, at, pair_at, step, count):
    got = lax.dot_general(picks, x, NT, preferred_element_type=F32)
    for k in range(count):
        stage[pl.ds(at + k * step, OWN, stride=PAD), :] = got[k * OWN : (k + 1) * OWN, 0:128]
    for p in range(count // 2):
        low = got[2 * p * OWN : (2 * p + 1) * OWN, 128:C]
        high = got[(2 * p + 1) * OWN : (2 * p + 2) * OWN, 128:C]
        stage[pl.ds(pair_at + p * step, OWN, stride=PAD), :] = jnp.concatenate([low, high], axis=1)


def unstage(stage, out_ref, rows):
    for d in range(OWN):
        out_ref[d] = stage[d * PAD : d * PAD + rows, :].astype(BF16)


def pack_priors(rank_ref, means_ref, logs_ref, out_ref, stage):
    picks = one_hot(rank_ref[...], 0, GRP, BF16)
    count = GRP // OWN

    def token(i, _):
        for which, ref in enumerate((means_ref, logs_ref)):
            at = which * PROWS + i
            pack_block(ref[i], picks, stage, at, at + count * TB, TB, count)
        return 0

    lax.fori_loop(0, TB, token, 0)
    unstage(stage, out_ref, 2 * PROWS)


def pack_latents(chunk, rank_ref, lat_ref, out_ref, stage):
    picks = one_hot(rank_ref[...], chunk * NU * OWN, NU * OWN, BF16)

    def frame(j, _):
        pack_block(lat_ref[j], picks, stage, j, j + NU * FB, FB, NU)
        return 0

    lax.fori_loop(0, FB, frame, 0)
    unstage(stage, out_ref, ROWS)


def build_sides(chunk, y_ref, text_ref, rhs_ref, bias_ref, wt, pr, zz, zs):
    wide = 152
    for s in range(OWN):
        m = y_ref[s, 0:PROWS, :].astype(F32)
        ls = y_ref[s, PROWS : 2 * PROWS, :].astype(F32)
        prec = jnp.exp(-2.0 * ls)
        wt[s * wide : s * wide + PROWS, :] = m * prec
        pr[s * wide : s * wide + PROWS, :] = prec
        zz[s * wide : s * wide + PROWS, :] = 0.5 * (m * m * prec) + ls
    rhs_ref[...] = jnp.zeros((NN, NK), BF16)
    lane = lax.broadcasted_iota(jnp.int32, (OWN, 128), 1)
    half = NK // 2 // 128
    count = GRP // OWN
    for i in range(TB):
        for k in range(NU):
            rows = pl.ds((chunk * NU + k) * TB + i, OWN, stride=wide)
            pairs = pl.ds((count + chunk * NU // 2 + k // 2) * TB + i, OWN, stride=wide)
            keep = (lane < 64) if k % 2 == 0 else (lane >= 64)
            at = slice(i * 128 + k * OWN, i * 128 + (k + 1) * OWN)
            for off, ref, scale in ((0, wt, 1.0), (half, pr, -0.5)):
                a = ref[rows, :].astype(BF16)
                b = jnp.where(keep, ref[pairs, :], 0.0).astype(BF16)
                q = (off + k) * 128
                rhs_ref[at, q : q + 128] = a * jnp.asarray(scale, BF16)
                q = (off + NU + k // 2) * 128
                rhs_ref[at, q : q + 128] = b * jnp.asarray(scale, BF16)
            zs[at, :] = zz[rows, :] + jnp.where(keep, zz[pairs, :], 0.0)
    ones = jnp.ones((8, 128), F32)
    lane8 = lax.broadcasted_iota(jnp.int32, (8, 128), 1)
    text = text_ref[...]
    for i in range(TB):
        total = lax.dot_general(
            ones, zs[i * 128 : (i + 1) * 128, :], NT, precision=lax.Precision.HIGHEST, preferred_element_type=F32
        )
        token = (lane8 % OWN) * TB + i
        bias_ref[:, i * 128 : (i + 1) * 128] = jnp.where(token < text, -total - C * HALF_LOG_TWO_PI, NEG)


def search(count_ref, y_ref, rhs_ref, bias_ref, text_ref, frame_ref, out_ref, lhs, lik, buf0, buf1):
    out_ref[...] = jnp.zeros(out_ref.shape, F32)
    blocks = NK // 2 // 128
    per = MB // FB

    def matmul_block(b, _):
        for q in range(per):
            s = b * per + q
            for k in range(blocks):
                x = y_ref[s, k * FB : (k + 1) * FB, :]
                lhs[q * FB : (q + 1) * FB, k * 128 : (k + 1) * 128] = x
                wide = x.astype(F32)
                lhs[q * FB : (q + 1) * FB, (blocks + k) * 128 : (blocks + k + 1) * 128] = (wide * wide).astype(BF16)
        for t in range(NN // 256):
            got = lax.dot_general(
                lhs[...], rhs_ref[t * 256 : (t + 1) * 256, :], NT, preferred_element_type=F32
            )
            bias = bias_ref[0:1, t * 256 : (t + 1) * 256]
            lik[pl.ds(b * (MB // 8), MB // 8), :, t * 256 : (t + 1) * 256] = (got + bias).reshape(MB // 8, 8, 256)
        return 0

    lax.fori_loop(0, count_ref[0], matmul_block, 0)

    lane = lax.broadcasted_iota(jnp.int32, (8, 128), 1)
    sub = lax.broadcasted_iota(jnp.int32, (8, 128), 0)
    block = lane % OWN
    seg = lane // OWN
    lane1 = lax.broadcasted_iota(jnp.int32, (1, 128), 1)
    first1 = (lane1 % OWN) == 0
    block_start = (block * TB).astype(F32)
    text = text_ref[...]
    frames = frame_ref[...]
    base = block * TB + frames - text
    inverse = 1.0 / (text - 1).astype(F32)
    scale = math.log2(math.e) / C

    def run_frames(at, state, buf, opening):
        for j in range(FB):
            entering = jnp.where(first1, opening if j == 0 else NEG, pltpu.roll(state[TB - 1], 1, 1))
            new = []
            for i in range(TB):
                like = lik[at + j // 8, j % 8 : j % 8 + 1, i * 128 : (i + 1) * 128]
                before = entering if i == 0 else state[i - 1]
                now = like + jnp.maximum(state[i], before)
                buf[j : j + 1, i * 128 : (i + 1) * 128] = now
                new.append(now)
            state = new
        return state

    def by_segment(x, reduce, fill):
        out = None
        for k in range(NU):
            one = reduce(jnp.where(seg == k, x, fill), axis=1, keepdims=True)
            out = jnp.broadcast_to(one, (8, 128)) if out is None else jnp.where(seg == k, one, out)
        return out

    def soften(index, buf, finish):
        rows = []
        for g in range(FB // 8):
            frame = index * FB + g * 8 + sub
            late = frame - base
            xs = [
                jnp.where(late <= i, buf[g * 8 : (g + 1) * 8, i * 128 : (i + 1) * 128], 8 * NEG)
                for i in range(TB)
            ]
            top = by_segment(functools.reduce(jnp.maximum, xs), jnp.max, -3.0e38)
            ws = [jnp.exp2((x - top) * scale) for x in xs]
            suffix = ws[TB - 1]
            moment = suffix
            for i in range(TB - 2, 0, -1):
                suffix = suffix + ws[i]
                moment = moment + suffix
            weight = suffix + ws[0]
            moment = moment + block_start * weight
            weight = by_segment(weight, jnp.sum, 0.0)
            moment = by_segment(moment, jnp.sum, 0.0)
            rows.append(jnp.where(frame < frames, moment / weight * inverse, 0.0))
            finish = finish + jnp.where(frame == frames - 1, top, 0.0)
        turned = jnp.concatenate(rows + [jnp.zeros((128 - FB, 128), F32)], axis=0).T
        where = jnp.maximum(index, 0)
        for k in range(NU):
            out_ref[where, k : k + 1, :] = turned[k * OWN : k * OWN + 1, :]
        return finish

    def pair(b, carried):
        state, finish = list(carried[:TB]), carried[TB]
        state = run_frames(b * (2 * FB // 8), state, buf0, jnp.where(b == 0, 0.0, NEG))
        finish = soften(2 * b - 1, buf1, finish)
        state = run_frames(b * (2 * FB // 8) + FB // 8, state, buf1, NEG)
        finish = soften(2 * b, buf0, finish)
        return (*state, finish)

    start = [jnp.full((1, 128), NEG, F32) for _ in range(TB)]
    carried = lax.fori_loop(0, count_ref[1], pair, (*start, jnp.zeros((8, 128), F32)))
    finish = soften(2 * count_ref[1] - 1, buf1, carried[TB])
    finish = jnp.sum(finish, axis=0, keepdims=True) * (1.0 / C)
    for d in range(OWN):
        out_ref[d, NU : NU + 1, :] = finish


def unpack(rank_ref, a_ref, b_ref, pos_ref, finish_ref, turned):
    lane1 = lax.broadcasted_iota(jnp.int32, (1, 128), 1)
    finish = jnp.zeros((1, 128), F32)
    for c, ref in enumerate((a_ref, b_ref)):
        rows = [ref[pl.ds(k, OWN, stride=8), :] for k in range(NU)]
        turned[:, c * 128 : (c + 1) * 128] = jnp.concatenate(rows, axis=0).T
        finish = finish + jnp.sum(ref[pl.ds(NU, OWN, stride=8), :], axis=0, keepdims=True)
    picks = one_hot(rank_ref[...], 0, GRP, F32)
    pos_ref[...] = lax.dot_general(
        turned[0:FB, :], picks, NN_DIMS, precision=lax.Precision.HIGHEST, preferred_element_type=F32
    )
    finish = jnp.sum(jnp.where(lane1 % OWN == 0, finish, 0.0), axis=1, keepdims=True)
    finish_ref[...] = jnp.broadcast_to(finish, (8, 128))


def exchange(x):
    return lax.all_to_all(x, SEQ, split_axis=0, concat_axis=0, tiled=True)


def make_rhs(chunk, prior, text_lanes):
    wide = pltpu.VMEM((OWN * 152, 128), F32)
    return call(
        functools.partial(build_sides, chunk),
        (jax.ShapeDtypeStruct((NN, NK), BF16), jax.ShapeDtypeStruct((8, NN), F32)),
        2,
        (wide, wide, wide, pltpu.VMEM((NN, 128), F32)),
    )(prior, text_lanes)


def run_search(counts, got, rhs, bias, text_lanes, frame_lanes):
    return call(
        search,
        jax.ShapeDtypeStruct((OWN, 8, 128), F32),
        6,
        (
            pltpu.VMEM((MB, NK), BF16),
            pltpu.VMEM((FR // 8, 8, NN), F32),
            pltpu.VMEM((FB, NN), F32),
            pltpu.VMEM((FB, NN), F32),
        ),
        smem=(0,),
    )(counts, got, rhs, bias, text_lanes, frame_lanes)


def pack_call(body, rank, arrays, rows):
    return call(
        body, jax.ShapeDtypeStruct((OWN, rows, 128), BF16), 1 + len(arrays), (pltpu.VMEM((OWN * PAD, 128), F32),)
    )(rank, *arrays)


def ranks(frame_lens):
    ids = jnp.arange(GRP, dtype=jnp.int32)
    a, b = frame_lens[:, None], frame_lens[None, :]
    ahead = (a > b) | ((a == b) & (ids[:, None] < ids[None, :]))
    return jnp.sum(ahead.astype(jnp.int32), axis=0)[None, :]


def owned(lens, rank, own):
    slots = jnp.arange(GRP // OWN, dtype=jnp.int32) * OWN + own
    return jnp.sum(jnp.where(rank == slots[:, None], lens[None, :], 0), axis=1)


def lanes_of(lens, chunk):
    part = lens[chunk * NU : (chunk + 1) * NU]
    return jnp.broadcast_to(jnp.repeat(part, OWN)[None, :], (8, 128))


def shards(means, log_scales, latents, text_lens, frame_lens):
    own = lax.axis_index(SEQ).astype(jnp.int32)
    rank = ranks(frame_lens)
    text_own, frame_own = owned(text_lens, rank, own), owned(frame_lens, rank, own)
    lat = jnp.transpose(latents, (1, 2, 0))
    turn = lambda x: jnp.transpose(x, (1, 2, 0))
    prior = exchange(pack_call(pack_priors, rank, (turn(means), turn(log_scales)), 2 * PROWS))
    got = [
        exchange(pack_call(functools.partial(pack_latents, c), rank, (lat,), ROWS)) for c in range(NCH)
    ]
    back = []
    for c in range(NCH):
        text_lanes, frame_lanes = lanes_of(text_own, c), lanes_of(frame_own, c)
        longest = jnp.max(frame_own[c * NU : (c + 1) * NU])
        counts = jnp.stack([(longest + MB - 1) // MB, (longest + 2 * FB - 1) // (2 * FB)])
        rhs, bias = make_rhs(c, prior, text_lanes)
        back.append(exchange(run_search(counts, got[c], rhs, bias, text_lanes, frame_lanes)))
    pos, finish = call(
        unpack,
        (jax.ShapeDtypeStruct((FB, GRP), F32), jax.ShapeDtypeStruct((8, 128), F32)),
        3,
        (pltpu.VMEM((128, 2 * 128), F32),),
    )(rank, *(b.reshape(OWN * 8, 128) for b in back))
    frame_total = lax.psum(jnp.sum(frame_lens).astype(F32), DP)
    path_total = lax.psum(finish[0, 0], DP)
    return (jnp.transpose(pos), -path_total / frame_total)


def solution(mesh):
    torus = Mesh(mesh.devices.reshape(4, 2, 4, 8), ("dp_0", "dp_1", "seq_0", "seq_1"))
    in_specs = (P(DP, SEQ, None), P(DP, SEQ, None), P(DP, SEQ, None), P(DP), P(DP))
    out_specs = (P(DP, SEQ), P())
    return jax.shard_map(
        shards, mesh=torus, in_specs=in_specs, out_specs=out_specs, check_vma=False
    )
```

```python
import functools
import math

import jax
import jax.numpy as jnp
from jax import lax
from jax.experimental import pallas as pl
from jax.experimental.pallas import tpu as pltpu
from jax.sharding import Mesh
from jax.sharding import PartitionSpec as P

SEQ = ("seq_0", "seq_1")
DP = ("dp_0", "dp_1")

C = 192
TXT = 384
FR = 1536
OWN = 32
GRP = 256
TB = TXT // OWN
FB = FR // OWN
NU = 4
NCH = GRP // OWN // NU
ROWS = (NU + NU // 2) * FB
PROWS = (GRP // OWN) * 3 // 2 * TB
PAD = 296
KP = 2 * 3 * 128
UNROLL = 4
NN = TB * 128
MB = 384

HALF_LOG_TWO_PI = 0.9189385332046727
NEG = -2.0e11
F32 = jnp.float32
BF16 = jnp.bfloat16
NT = (((1,), (1,)), ((), ()))
NN_DIMS = (((1,), (0,)), ((), ()))


def params():
    return pltpu.CompilerParams(vmem_limit_bytes=60 * 1024 * 1024)


def call(body, out_shape, n_in, scratch=(), smem=()):
    vmem = pl.BlockSpec(memory_space=pltpu.VMEM)
    return pl.pallas_call(
        body,
        out_shape=out_shape,
        in_specs=[pl.BlockSpec(memory_space=pltpu.SMEM) if i in smem else vmem for i in range(n_in)],
        out_specs=jax.tree.map(lambda _: vmem, out_shape),
        scratch_shapes=list(scratch),
        compiler_params=params(),
    )


def one_hot(rank_row, first, count, dtype):
    ids = lax.broadcasted_iota(jnp.int32, (count, GRP), 0) + first
    return jnp.where(ids == rank_row, 1.0, 0.0).astype(dtype)


def pack_block(x, picks, stage, at, pair_at, step, count):
    got = lax.dot_general(picks, x, NT, preferred_element_type=F32)
    for k in range(count):
        stage[pl.ds(at + k * step, OWN, stride=PAD), :] = got[k * OWN : (k + 1) * OWN, 0:128]
    for p in range(count // 2):
        low = got[2 * p * OWN : (2 * p + 1) * OWN, 128:C]
        high = got[(2 * p + 1) * OWN : (2 * p + 2) * OWN, 128:C]
        stage[pl.ds(pair_at + p * step, OWN, stride=PAD), :] = jnp.concatenate([low, high], axis=1)


def unstage(stage, out_ref, rows):
    for d in range(OWN):
        out_ref[d] = stage[d * PAD : d * PAD + rows, :].astype(BF16)


def stage_priors(rank_ref, means_ref, logs_ref, stage):
    picks = one_hot(rank_ref[...], 0, GRP, BF16)
    count = GRP // OWN

    def tokens(i, _):
        for q in range(UNROLL // 2):
            for which, ref in enumerate((means_ref, logs_ref)):
                token = i * (UNROLL // 2) + q
                at = which * PROWS + token
                pack_block(ref[token], picks, stage, at, at + count * TB, TB, count)
        return 0

    lax.fori_loop(0, 2 * TB // UNROLL, tokens, 0)


def stage_latents(chunk, rank_ref, lat_ref, stage):
    picks = one_hot(rank_ref[...], chunk * NU * OWN, NU * OWN, BF16)

    def frames(j, _):
        for q in range(UNROLL):
            frame = j * UNROLL + q
            pack_block(lat_ref[frame], picks, stage, frame, frame + NU * FB, FB, NU)
        return 0

    lax.fori_loop(0, FB // UNROLL, frames, 0)


def unstage(stage, out_ref, first, rows):
    for d in range(OWN):
        out_ref[d, first : first + rows, :] = stage[d * PAD : d * PAD + rows, :].astype(BF16)


def pack_first(rank_ref, means_ref, logs_ref, lat_ref, out_ref, stage):
    stage_priors(rank_ref, means_ref, logs_ref, stage)
    unstage(stage, out_ref, 0, 2 * PROWS)
    stage_latents(0, rank_ref, lat_ref, stage)
    unstage(stage, out_ref, 2 * PROWS, ROWS)


def pack_second(rank_ref, lat_ref, out_ref, stage):
    stage_latents(1, rank_ref, lat_ref, stage)
    unstage(stage, out_ref, 0, ROWS)


def build_sides(y_ref, text_ref, rhs_ref, bias_ref, wt, pr, zz, zs):
    wide = 152
    for s in range(OWN):
        m = y_ref[s, 0:PROWS, :].astype(F32)
        ls = y_ref[s, PROWS : 2 * PROWS, :].astype(F32)
        prec = jnp.exp(-2.0 * ls)
        wt[s * wide : s * wide + PROWS, :] = m * prec
        pr[s * wide : s * wide + PROWS, :] = prec
        zz[s * wide : s * wide + PROWS, :] = 0.5 * (m * m * prec) + ls
    lane = lax.broadcasted_iota(jnp.int32, (OWN, 128), 1)
    none = jnp.zeros((OWN, 128), F32)
    ones = jnp.ones((8, 128), F32)
    lane8 = lax.broadcasted_iota(jnp.int32, (8, 128), 1)
    count = GRP // OWN

    def rows_of(ref, block, i):
        return ref[pl.ds(block * TB + i, OWN, stride=wide), :]

    def both(ref, pair, i):
        x = rows_of(ref, count + pair, i)
        return [jnp.where(lane < 64, x, 0.0), jnp.where(lane >= 64, x, 0.0)]

    for pair in range(count // 2):
        c, p = pair // 2, pair % 2
        for v in range(TB // 2):
            for half, (ref, factor) in enumerate(((wt, 1.0), (pr, -0.5))):
                first, second, mixed = [], [], []
                for i in (2 * v, 2 * v + 1):
                    first += [rows_of(ref, 2 * pair, i), none]
                    second += [none, rows_of(ref, 2 * pair + 1, i)]
                    mixed += both(ref, pair, i)
                for q, pieces in enumerate((first, second, mixed)):
                    turned = jnp.concatenate(pieces, axis=0).T.astype(BF16)
                    k = (half * 3 + q) * 128
                    rhs_ref[pair, k : k + 128, v * 128 : (v + 1) * 128] = turned * jnp.asarray(factor, BF16)
        for i in range(TB):
            for k, extra in enumerate(both(zz, pair, i)):
                at = c * NN + i * 128 + (2 * p + k) * OWN
                zs[at : at + OWN, :] = rows_of(zz, 2 * pair + k, i) + extra
    for c in range(NCH):
        text = text_ref[c]
        for i in range(TB):
            total = lax.dot_general(
                ones,
                zs[c * NN + i * 128 : c * NN + (i + 1) * 128, :],
                NT,
                precision=lax.Precision.HIGHEST,
                preferred_element_type=F32,
            )
            token = (lane8 % OWN) * TB + i
            bias_ref[c, :, i * 128 : (i + 1) * 128] = jnp.where(
                token < text, -total - C * HALF_LOG_TWO_PI, NEG
            )


def search(chunk, first_row, count_ref, y_ref, rhs_ref, bias_ref, text_ref, frame_ref, *rest):
    earlier, (out_ref, lhs, lik, buf0, buf1) = rest[:-5], rest[-5:]
    out_ref[...] = earlier[0][...] if earlier else jnp.zeros(out_ref.shape, F32)
    per = MB // FB
    wide_lane = lax.broadcasted_iota(jnp.int32, (MB, 128), 1)

    def matmul_block(b, _):
        for q in range(per):
            s = b * per + q
            rows = slice(q * FB, (q + 1) * FB)
            for p in range(NU // 2):
                for n, k in enumerate((2 * p, 2 * p + 1, NU + p)):
                    x = y_ref[s, first_row + k * FB : first_row + (k + 1) * FB, :]
                    at = p * KP + n * 128
                    lhs[rows, at : at + 128] = x
                    wide = x.astype(F32)
                    lhs[rows, at + 384 : at + 512] = (wide * wide).astype(BF16)
        group = pl.ds(b * (MB // 8), MB // 8)
        for t in range(KP // 256):
            got = [
                lax.dot_general(
                    lhs[:, p * KP : (p + 1) * KP],
                    rhs_ref[chunk * 2 + p, :, t * 256 : (t + 1) * 256],
                    NN_DIMS,
                    preferred_element_type=F32,
                )
                for p in range(2)
            ]
            for h in range(2):
                one, two = (g[:, h * 128 : (h + 1) * 128] for g in got)
                i = 4 * t + 2 * h
                even = jnp.where(wide_lane < 64, one, pltpu.roll(two, 64, 1))
                odd = jnp.where(wide_lane < 64, pltpu.roll(one, 64, 1), two)
                for n, x in enumerate((even, odd)):
                    cols = slice((i + n) * 128, (i + n + 1) * 128)
                    lik[group, :, cols] = (x + bias_ref[chunk, 0:1, cols]).reshape(MB // 8, 8, 128)
        return 0

    lax.fori_loop(0, count_ref[chunk], matmul_block, 0)

    lane = lax.broadcasted_iota(jnp.int32, (8, 128), 1)
    sub = lax.broadcasted_iota(jnp.int32, (8, 128), 0)
    block = lane % OWN
    seg = lane // OWN
    lane1 = lax.broadcasted_iota(jnp.int32, (1, 128), 1)
    first1 = (lane1 % OWN) == 0
    block_start = (block * TB).astype(F32)
    text = text_ref[chunk]
    frames = frame_ref[chunk]
    base = block * TB + frames - text
    inverse = 1.0 / (text - 1).astype(F32)
    scale = math.log2(math.e) / C

    def run_frames(at, state, buf, opening):
        for j in range(FB):
            entering = jnp.where(first1, opening if j == 0 else NEG, pltpu.roll(state[TB - 1], 1, 1))
            new = []
            for i in range(TB):
                like = lik[at + j // 8, j % 8 : j % 8 + 1, i * 128 : (i + 1) * 128]
                before = entering if i == 0 else state[i - 1]
                now = like + jnp.maximum(state[i], before)
                buf[j : j + 1, i * 128 : (i + 1) * 128] = now
                new.append(now)
            state = new
        return state

    def by_segment(x, reduce, fill):
        out = None
        for k in range(NU):
            one = reduce(jnp.where(seg == k, x, fill), axis=1, keepdims=True)
            out = jnp.broadcast_to(one, (8, 128)) if out is None else jnp.where(seg == k, one, out)
        return out

    def soften(index, buf, finish):
        rows = []
        for g in range(FB // 8):
            frame = index * FB + g * 8 + sub
            late = frame - base
            xs = [
                jnp.where(late <= i, buf[g * 8 : (g + 1) * 8, i * 128 : (i + 1) * 128], 8 * NEG)
                for i in range(TB)
            ]
            top = by_segment(functools.reduce(jnp.maximum, xs), jnp.max, -3.0e38)
            ws = [jnp.exp2((x - top) * scale) for x in xs]
            suffix = ws[TB - 1]
            moment = suffix
            for i in range(TB - 2, 0, -1):
                suffix = suffix + ws[i]
                moment = moment + suffix
            weight = suffix + ws[0]
            moment = moment + block_start * weight
            weight = by_segment(weight, jnp.sum, 0.0)
            moment = by_segment(moment, jnp.sum, 0.0)
            rows.append(jnp.where(frame < frames, moment / weight * inverse, 0.0))
            finish = finish + jnp.where(frame == frames - 1, top, 0.0)
        turned = jnp.concatenate(rows + [jnp.zeros((128 - FB, 128), F32)], axis=0).T
        where = jnp.maximum(index, 0)
        for k in range(NU):
            out_ref[where, chunk * NU + k : chunk * NU + k + 1, :] = turned[k * OWN : k * OWN + 1, :]
        return finish

    def pair(b, carried):
        state, finish = list(carried[:TB]), carried[TB]
        state = run_frames(b * (2 * FB // 8), state, buf0, jnp.where(b == 0, 0.0, NEG))
        finish = soften(2 * b - 1, buf1, finish)
        state = run_frames(b * (2 * FB // 8) + FB // 8, state, buf1, NEG)
        finish = soften(2 * b, buf0, finish)
        return (*state, finish)

    start = [jnp.full((1, 128), NEG, F32) for _ in range(TB)]
    carried = lax.fori_loop(0, count_ref[NCH + chunk], pair, (*start, jnp.zeros((8, 128), F32)))
    finish = soften(2 * count_ref[NCH + chunk] - 1, buf1, carried[TB])
    finish = jnp.sum(finish, axis=0, keepdims=True) * (1.0 / C)
    finish = jnp.sum(jnp.where(first1, finish, 0.0), axis=1, keepdims=True)
    for d in range(OWN):
        out_ref[d, chunk * NU : chunk * NU + 1, 64:128] = jnp.broadcast_to(finish, (1, 64))


def unpack(rank_ref, frame_ref, got_ref, pos_ref, sums_ref, turned):
    lane1 = lax.broadcasted_iota(jnp.int32, (1, 128), 1)
    rows = [got_ref[pl.ds(k, OWN, stride=8), :] for k in range(NCH * NU)]
    finish = sum(jnp.sum(rows[c * NU], axis=0, keepdims=True) for c in range(NCH))
    for c in range(2):
        turned[:, c * 128 : (c + 1) * 128] = jnp.concatenate(rows[c * 4 : c * 4 + 4], axis=0).T
    picks = one_hot(rank_ref[...], 0, GRP, F32)
    pos_ref[...] = lax.dot_general(
        turned[0:FB, :], picks, NN_DIMS, precision=lax.Precision.HIGHEST, preferred_element_type=F32
    )
    lens = jnp.sum(frame_ref[...].astype(F32), axis=1, keepdims=True)
    sums = jnp.where(lane1 >= 64, finish, lens)
    sums_ref[...] = jnp.broadcast_to(sums, (8, 128))


def exchange(x):
    return lax.all_to_all(x, SEQ, split_axis=0, concat_axis=0, tiled=True)


def make_rhs(first, text_lanes):
    wide = pltpu.VMEM((OWN * 152, 128), F32)
    return call(
        build_sides,
        (jax.ShapeDtypeStruct((NCH * 2, KP, KP), BF16), jax.ShapeDtypeStruct((NCH, 8, NN), F32)),
        2,
        (wide, wide, wide, pltpu.VMEM((NCH * NN, 128), F32)),
    )(first, text_lanes)


def run_search(chunk, first_row, *operands):
    return call(
        functools.partial(search, chunk, first_row),
        jax.ShapeDtypeStruct((OWN, 8, 128), F32),
        len(operands),
        (
            pltpu.VMEM((MB, 2 * KP), BF16),
            pltpu.VMEM((FR // 8, 8, NN), F32),
            pltpu.VMEM((FB, NN), F32),
            pltpu.VMEM((FB, NN), F32),
        ),
        smem=(0,),
    )(*operands)


def pack_call(body, rows, *operands):
    return call(
        body,
        jax.ShapeDtypeStruct((OWN, rows, 128), BF16),
        len(operands),
        (pltpu.VMEM((OWN * PAD, 128), F32),),
    )(*operands)


def ranks(frame_lens):
    ids = jnp.arange(GRP, dtype=jnp.int32)
    a, b = frame_lens[:, None], frame_lens[None, :]
    ahead = (a > b) | ((a == b) & (ids[:, None] < ids[None, :]))
    return jnp.sum(ahead.astype(jnp.int32), axis=0)[None, :]


def owned(lens, rank, own):
    slots = jnp.arange(GRP // OWN, dtype=jnp.int32) * OWN + own
    return jnp.sum(jnp.where(rank == slots[:, None], lens[None, :], 0), axis=1)


def lanes_of(lens):
    parts = jnp.repeat(lens.reshape(NCH, 1, NU), OWN, axis=2)
    return jnp.broadcast_to(parts, (NCH, 8, 128))


def counts_of(frame_own):
    longest = jnp.max(frame_own.reshape(NCH, NU), axis=1)
    return jnp.concatenate([(longest + MB - 1) // MB, (longest + 2 * FB - 1) // (2 * FB)])


def over_groups(x):
    x = x + lax.ppermute(x, "dp_1", [(0, 1), (1, 0)])
    turns = [lax.ppermute(x, "dp_0", [(i, (i + n) % 4) for i in range(4)]) for n in (1, 2, 3)]
    return x + turns[0] + turns[1] + turns[2]


def shards(means, log_scales, latents, text_lens, frame_lens):
    own = lax.axis_index(SEQ).astype(jnp.int32)
    rank = ranks(frame_lens)
    text_own, frame_own = owned(text_lens, rank, own), owned(frame_lens, rank, own)
    means, log_scales, latents = (jnp.transpose(x, (1, 2, 0)) for x in (means, log_scales, latents))
    first = exchange(pack_call(pack_first, 2 * PROWS + ROWS, rank, means, log_scales, latents))
    second = exchange(pack_call(pack_second, ROWS, rank, latents))
    text_lanes, frame_lanes, counts = lanes_of(text_own), lanes_of(frame_own), counts_of(frame_own)
    sides = (*make_rhs(first, text_lanes), text_lanes, frame_lanes)
    back = run_search(0, 2 * PROWS, counts, first, *sides)
    back = exchange(run_search(1, 0, counts, second, *sides, back))
    pos, sums = call(
        unpack,
        (jax.ShapeDtypeStruct((FB, GRP), F32), jax.ShapeDtypeStruct((8, 128), F32)),
        3,
        (pltpu.VMEM((128, 2 * 128), F32),),
    )(rank, frame_lens[None, :], back.reshape(OWN * 8, 128))
    sums = over_groups(sums)
    return (jnp.transpose(pos), -sums[0, 64] / sums[0, 0])


def solution(mesh):
    torus = Mesh(mesh.devices.reshape(4, 2, 4, 8), ("dp_0", "dp_1", "seq_0", "seq_1"))
    in_specs = (P(DP, SEQ, None), P(DP, SEQ, None), P(DP, SEQ, None), P(DP), P(DP))
    out_specs = (P(DP, SEQ), P())
    return jax.shard_map(
        shards, mesh=torus, in_specs=in_specs, out_specs=out_specs, check_vma=False
    )
```

```python
import functools
import math

import jax
import jax.numpy as jnp
from jax import lax
from jax.experimental import pallas as pl
from jax.experimental.pallas import tpu as pltpu
from jax.sharding import Mesh
from jax.sharding import PartitionSpec as P

SEQ = ("seq_0", "seq_1")
DP = ("dp_0", "dp_1")

C = 192
TXT = 384
FR = 1536
OWN = 32
GRP = 256
TB = TXT // OWN
FB = FR // OWN
NU = 4
NCH = GRP // OWN // NU
ROWS = (NU + NU // 2) * FB
PROWS = (GRP // OWN) * 3 // 2 * TB
PAD = 296
KP = 2 * 3 * 128
FRAME_UNROLL = 16
TOKEN_UNROLL = 6
NN = TB * 128
MB = 384

HALF_LOG_TWO_PI = 0.9189385332046727
NEG = -2.0e11
F32 = jnp.float32
BF16 = jnp.bfloat16
NT = (((1,), (1,)), ((), ()))
NN_DIMS = (((1,), (0,)), ((), ()))


def call(body, out_shape, n_in, scratch=(), smem=(), mib=24):
    vmem = pl.BlockSpec(memory_space=pltpu.VMEM)
    return pl.pallas_call(
        body,
        out_shape=out_shape,
        in_specs=[pl.BlockSpec(memory_space=pltpu.SMEM) if i in smem else vmem for i in range(n_in)],
        out_specs=jax.tree.map(lambda _: vmem, out_shape),
        scratch_shapes=list(scratch),
        compiler_params=pltpu.CompilerParams(vmem_limit_bytes=mib * 1024 * 1024),
    )


def one_hot(rank_row, first, count, dtype):
    ids = lax.broadcasted_iota(jnp.int32, (count, GRP), 0) + first
    return jnp.where(ids == rank_row, 1.0, 0.0).astype(dtype)


def pack_block(x, picks, stage, at, pair_at, step, count):
    got = lax.dot_general(picks, x, NT, preferred_element_type=F32)
    for k in range(count):
        stage[pl.ds(at + k * step, OWN, stride=PAD), :] = got[k * OWN : (k + 1) * OWN, 0:128]
    for p in range(count // 2):
        low = got[2 * p * OWN : (2 * p + 1) * OWN, 128:C]
        high = got[(2 * p + 1) * OWN : (2 * p + 2) * OWN, 128:C]
        stage[pl.ds(pair_at + p * step, OWN, stride=PAD), :] = jnp.concatenate([low, high], axis=1)


def stage_priors(rank_ref, means_ref, logs_ref, stage):
    picks = one_hot(rank_ref[...], 0, GRP, BF16)
    count = GRP // OWN

    def tokens(i, _):
        for q in range(TOKEN_UNROLL):
            for which, ref in enumerate((means_ref, logs_ref)):
                token = i * TOKEN_UNROLL + q
                at = which * PROWS + token
                pack_block(ref[token], picks, stage, at, at + count * TB, TB, count)
        return 0

    lax.fori_loop(0, TB // TOKEN_UNROLL, tokens, 0)


def stage_latents(chunk, rank_ref, lat_ref, stage):
    picks = one_hot(rank_ref[...], chunk * NU * OWN, NU * OWN, BF16)

    def frames(j, _):
        for q in range(FRAME_UNROLL):
            frame = j * FRAME_UNROLL + q
            pack_block(lat_ref[frame], picks, stage, frame, frame + NU * FB, FB, NU)
        return 0

    lax.fori_loop(0, FB // FRAME_UNROLL, frames, 0)


def unstage(stage, out_ref, first, rows):
    for d in range(OWN):
        out_ref[d, first : first + rows, :] = stage[d * PAD : d * PAD + rows, :].astype(BF16)


def pack_first(rank_ref, means_ref, logs_ref, lat_ref, out_ref, stage):
    stage_priors(rank_ref, means_ref, logs_ref, stage)
    unstage(stage, out_ref, 0, 2 * PROWS)
    stage_latents(0, rank_ref, lat_ref, stage)
    unstage(stage, out_ref, 2 * PROWS, ROWS)


def pack_second(rank_ref, lat_ref, out_ref, stage):
    stage_latents(1, rank_ref, lat_ref, stage)
    unstage(stage, out_ref, 0, ROWS)


def build_sides(y_ref, text_ref, rhs0_ref, rhs1_ref, bias0_ref, bias1_ref, wt, pr, zz, zs):
    wide = 152
    for s in range(OWN):
        m = y_ref[s, 0:PROWS, :].astype(F32)
        ls = y_ref[s, PROWS : 2 * PROWS, :].astype(F32)
        prec = jnp.exp(-2.0 * ls)
        wt[s * wide : s * wide + PROWS, :] = m * prec
        pr[s * wide : s * wide + PROWS, :] = prec
        zz[s * wide : s * wide + PROWS, :] = 0.5 * (m * m * prec) + ls
    lane = lax.broadcasted_iota(jnp.int32, (OWN, 128), 1)
    none = jnp.zeros((OWN, 128), F32)
    ones = jnp.ones((8, 128), F32)
    lane8 = lax.broadcasted_iota(jnp.int32, (8, 128), 1)
    count = GRP // OWN

    def rows_of(ref, block, i):
        return ref[pl.ds(block * TB + i, OWN, stride=wide), :]

    def both(ref, pair, i):
        x = rows_of(ref, count + pair, i)
        return [jnp.where(lane < 64, x, 0.0), jnp.where(lane >= 64, x, 0.0)]

    for pair in range(count // 2):
        c, p = pair // 2, pair % 2
        for v in range(TB // 2):
            for half, (ref, factor) in enumerate(((wt, 1.0), (pr, -0.5))):
                first, second, mixed = [], [], []
                for i in (2 * v, 2 * v + 1):
                    first += [rows_of(ref, 2 * pair, i), none]
                    second += [none, rows_of(ref, 2 * pair + 1, i)]
                    mixed += both(ref, pair, i)
                for q, pieces in enumerate((first, second, mixed)):
                    turned = jnp.concatenate(pieces, axis=0).T.astype(BF16)
                    k = (half * 3 + q) * 128
                    (rhs0_ref, rhs1_ref)[c][p, k : k + 128, v * 128 : (v + 1) * 128] = turned * jnp.asarray(factor, BF16)
        for i in range(TB):
            for k, extra in enumerate(both(zz, pair, i)):
                at = c * NN + i * 128 + (2 * p + k) * OWN
                zs[at : at + OWN, :] = rows_of(zz, 2 * pair + k, i) + extra
    for c in range(NCH):
        text = text_ref[c]
        for i in range(TB):
            total = lax.dot_general(
                ones,
                zs[c * NN + i * 128 : c * NN + (i + 1) * 128, :],
                NT,
                precision=lax.Precision.HIGHEST,
                preferred_element_type=F32,
            )
            token = (lane8 % OWN) * TB + i
            (bias0_ref, bias1_ref)[c][:, i * 128 : (i + 1) * 128] = jnp.where(
                token < text, -total - C * HALF_LOG_TWO_PI, NEG
            )


def search(chunk, first_row, count_ref, y_ref, rhs_ref, bias_ref, text_ref, frame_ref, *rest):
    earlier, (out_ref, lhs, lik, buf0, buf1) = rest[:-5], rest[-5:]
    out_ref[...] = earlier[0][...] if earlier else jnp.zeros(out_ref.shape, F32)
    per = MB // FB
    wide_lane = lax.broadcasted_iota(jnp.int32, (MB, 128), 1)

    def matmul_block(b, _):
        for q in range(per):
            s = b * per + q
            rows = slice(q * FB, (q + 1) * FB)
            for p in range(NU // 2):
                for n, k in enumerate((2 * p, 2 * p + 1, NU + p)):
                    x = y_ref[s, first_row + k * FB : first_row + (k + 1) * FB, :]
                    at = p * KP + n * 128
                    lhs[rows, at : at + 128] = x
                    wide = x.astype(F32)
                    lhs[rows, at + 384 : at + 512] = (wide * wide).astype(BF16)
        group = pl.ds(b * (MB // 8), MB // 8)
        for t in range(KP // 256):
            got = [
                lax.dot_general(
                    lhs[:, p * KP : (p + 1) * KP],
                    rhs_ref[p, :, t * 256 : (t + 1) * 256],
                    NN_DIMS,
                    preferred_element_type=F32,
                )
                for p in range(2)
            ]
            for h in range(2):
                one, two = (g[:, h * 128 : (h + 1) * 128] for g in got)
                i = 4 * t + 2 * h
                even = jnp.where(wide_lane < 64, one, pltpu.roll(two, 64, 1))
                odd = jnp.where(wide_lane < 64, pltpu.roll(one, 64, 1), two)
                for n, x in enumerate((even, odd)):
                    cols = slice((i + n) * 128, (i + n + 1) * 128)
                    lik[group, :, cols] = (x + bias_ref[0:1, cols]).reshape(MB // 8, 8, 128)
        return 0

    lax.fori_loop(0, count_ref[chunk], matmul_block, 0)

    lane = lax.broadcasted_iota(jnp.int32, (8, 128), 1)
    sub = lax.broadcasted_iota(jnp.int32, (8, 128), 0)
    block = lane % OWN
    seg = lane // OWN
    lane1 = lax.broadcasted_iota(jnp.int32, (1, 128), 1)
    first1 = (lane1 % OWN) == 0
    block_start = (block * TB).astype(F32)
    text = text_ref[chunk]
    frames = frame_ref[chunk]
    base = block * TB + frames - text
    inverse = 1.0 / (text - 1).astype(F32)
    scale = math.log2(math.e) / C

    def run_frames(at, state, buf, opening):
        for j in range(FB):
            entering = jnp.where(first1, opening if j == 0 else NEG, pltpu.roll(state[TB - 1], 1, 1))
            new = []
            for i in range(TB):
                like = lik[at + j // 8, j % 8 : j % 8 + 1, i * 128 : (i + 1) * 128]
                before = entering if i == 0 else state[i - 1]
                now = like + jnp.maximum(state[i], before)
                buf[j : j + 1, i * 128 : (i + 1) * 128] = now
                new.append(now)
            state = new
        return state

    def by_segment(x, reduce, fill):
        out = None
        for k in range(NU):
            one = reduce(jnp.where(seg == k, x, fill), axis=1, keepdims=True)
            out = jnp.broadcast_to(one, (8, 128)) if out is None else jnp.where(seg == k, one, out)
        return out

    seg_rows = lax.broadcasted_iota(jnp.int32, (128, 128), 0) // OWN
    seg_cols = lax.broadcasted_iota(jnp.int32, (128, 128), 1) // OWN
    same = jnp.where(seg_rows == seg_cols, 1.0, 0.0).astype(BF16)

    def over_segment(x):
        high = x.astype(BF16)
        rest = x - high.astype(F32)
        mid = rest.astype(BF16)
        low = (rest - mid.astype(F32)).astype(BF16)
        parts = [lax.dot_general(y, same, NN_DIMS, preferred_element_type=F32) for y in (high, mid, low)]
        return parts[0] + (parts[1] + parts[2])

    def soften(index, buf, finish):
        frame = index * FB + lax.broadcasted_iota(jnp.int32, (FB, 128), 0)
        weights, moments, tops = [], [], []
        for g in range(FB // 8):
            late = index * FB + g * 8 + sub - base
            xs = [
                jnp.where(late <= i, buf[g * 8 : (g + 1) * 8, i * 128 : (i + 1) * 128], 8 * NEG)
                for i in range(TB)
            ]
            top = by_segment(functools.reduce(jnp.maximum, xs), jnp.max, -3.0e38)
            ws = [jnp.exp2((x - top) * scale) for x in xs]
            suffix = ws[TB - 1]
            moment = suffix
            for i in range(TB - 2, 0, -1):
                suffix = suffix + ws[i]
                moment = moment + suffix
            weight = suffix + ws[0]
            weights.append(weight)
            moments.append(moment + block_start * weight)
            tops.append(top)
        weight, moment = (over_segment(jnp.concatenate(x, axis=0)) for x in (weights, moments))
        place = jnp.where(frame < frames[0:1], moment / weight * inverse[0:1], 0.0)
        ended = jnp.where(frame == frames[0:1] - 1, jnp.concatenate(tops, axis=0), 0.0)
        finish = finish + jnp.sum(ended.reshape(FB // 8, 8, 128), axis=0)
        rows = [place]
        turned = jnp.concatenate(rows + [jnp.zeros((128 - FB, 128), F32)], axis=0).T
        where = jnp.maximum(index, 0)
        for k in range(NU):
            out_ref[where, chunk * NU + k : chunk * NU + k + 1, :] = turned[k * OWN : k * OWN + 1, :]
        return finish

    def pair(b, carried):
        state, finish = list(carried[:TB]), carried[TB]
        state = run_frames(b * (2 * FB // 8), state, buf0, jnp.where(b == 0, 0.0, NEG))
        finish = soften(2 * b - 1, buf1, finish)
        state = run_frames(b * (2 * FB // 8) + FB // 8, state, buf1, NEG)
        finish = soften(2 * b, buf0, finish)
        return (*state, finish)

    start = [jnp.full((1, 128), NEG, F32) for _ in range(TB)]
    carried = lax.fori_loop(0, count_ref[NCH + chunk], pair, (*start, jnp.zeros((8, 128), F32)))
    finish = soften(2 * count_ref[NCH + chunk] - 1, buf1, carried[TB])
    finish = jnp.sum(finish, axis=0, keepdims=True) * (1.0 / C)
    finish = jnp.sum(jnp.where(first1, finish, 0.0), axis=1, keepdims=True)
    for d in range(OWN):
        out_ref[d, chunk * NU : chunk * NU + 1, 64:128] = jnp.broadcast_to(finish, (1, 64))


def unpack(rank_ref, got_ref, pos_ref, turned):
    rows = [got_ref[pl.ds(k, OWN, stride=8), :] for k in range(NCH * NU)]
    for c in range(2):
        turned[:, c * 128 : (c + 1) * 128] = jnp.concatenate(rows[c * 4 : c * 4 + 4], axis=0).T
    picks = one_hot(rank_ref[...], 0, GRP, F32)
    pos_ref[...] = lax.dot_general(
        turned[0:FB, :], picks, NN_DIMS, precision=lax.Precision.HIGHEST, preferred_element_type=F32
    )


def sum_up(back, frame_lens):
    finish = jnp.sum(back, axis=(0, 1), keepdims=True)[0]
    lens = jnp.sum(frame_lens).astype(F32)
    lanes = lax.broadcasted_iota(jnp.int32, (1, 128), 1)
    return jnp.where(lanes >= 64, finish, lens)


def exchange(x):
    return lax.all_to_all(x, SEQ, split_axis=0, concat_axis=0, tiled=True)


def make_rhs(first, text_lanes):
    wide = pltpu.VMEM((OWN * 152, 128), F32)
    return call(
        build_sides,
        (jax.ShapeDtypeStruct((2, KP, KP), BF16),) * NCH + (jax.ShapeDtypeStruct((8, NN), F32),) * NCH,
        2,
        (wide, wide, wide, pltpu.VMEM((NCH * NN, 128), F32)),
        mib=32,
    )(first, text_lanes)


def run_search(chunk, first_row, *operands):
    return call(
        functools.partial(search, chunk, first_row),
        jax.ShapeDtypeStruct((OWN, 8, 128), F32),
        len(operands),
        (
            pltpu.VMEM((MB, 2 * KP), BF16),
            pltpu.VMEM((FR // 8, 8, NN), F32),
            pltpu.VMEM((FB, NN), F32),
            pltpu.VMEM((FB, NN), F32),
        ),
        smem=(0,),
    )(*operands)


def pack_call(body, rows, *operands):
    return call(
        body,
        jax.ShapeDtypeStruct((OWN, rows, 128), BF16),
        len(operands),
        (pltpu.VMEM((OWN * PAD, 128), F32),),
    )(*operands)


def ranks(frame_lens):
    ids = jnp.arange(GRP, dtype=jnp.int32)
    a, b = frame_lens[:, None], frame_lens[None, :]
    ahead = (a > b) | ((a == b) & (ids[:, None] < ids[None, :]))
    return jnp.sum(ahead.astype(jnp.int32), axis=0)[None, :]


def owned(lens, rank, own):
    slots = jnp.arange(GRP // OWN, dtype=jnp.int32) * OWN + own
    return jnp.sum(jnp.where(rank == slots[:, None], lens[None, :], 0), axis=1)


def lanes_of(lens):
    parts = jnp.repeat(lens.reshape(NCH, 1, NU), OWN, axis=2)
    return jnp.broadcast_to(parts, (NCH, 8, 128))


def counts_of(frame_own):
    longest = jnp.max(frame_own.reshape(NCH, NU), axis=1)
    return jnp.concatenate([(longest + MB - 1) // MB, (longest + 2 * FB - 1) // (2 * FB)])


def over_groups(x):
    x = x + lax.ppermute(x, "dp_1", [(0, 1), (1, 0)])
    for n in (1, 2):
        x = x + lax.ppermute(x, "dp_0", [(i, (i + n) % 4) for i in range(4)])
    return x


def shards(means, log_scales, latents, text_lens, frame_lens):
    own = lax.axis_index(SEQ).astype(jnp.int32)
    rank = ranks(frame_lens)
    text_own, frame_own = owned(text_lens, rank, own), owned(frame_lens, rank, own)
    means, log_scales, latents = (jnp.transpose(x, (1, 2, 0)) for x in (means, log_scales, latents))
    first = exchange(pack_call(pack_first, 2 * PROWS + ROWS, rank, means, log_scales, latents))
    second = exchange(pack_call(pack_second, ROWS, rank, latents))
    text_lanes, frame_lanes, counts = lanes_of(text_own), lanes_of(frame_own), counts_of(frame_own)
    rhs0, rhs1, bias0, bias1 = make_rhs(first, text_lanes)
    back = run_search(0, 2 * PROWS, counts, first, rhs0, bias0, text_lanes, frame_lanes)
    back = exchange(run_search(1, 0, counts, second, rhs1, bias1, text_lanes, frame_lanes, back))
    sums = over_groups(sum_up(back, frame_lens))
    pos = call(
        unpack, jax.ShapeDtypeStruct((FB, GRP), F32), 2, (pltpu.VMEM((128, 2 * 128), F32),)
    )(rank, back.reshape(OWN * 8, 128))
    return (jnp.transpose(pos), -sums[0, 64] / sums[0, 0])


def solution(mesh):
    torus = Mesh(mesh.devices.reshape(4, 2, 4, 8), ("dp_0", "dp_1", "seq_0", "seq_1"))
    in_specs = (P(DP, SEQ, None), P(DP, SEQ, None), P(DP, SEQ, None), P(DP), P(DP))
    out_specs = (P(DP, SEQ), P())
    return jax.shard_map(
        shards, mesh=torus, in_specs=in_specs, out_specs=out_specs, check_vma=False
    )
```

```python
import functools
import math

import jax
import jax.numpy as jnp
from jax import lax
from jax.experimental import pallas as pl
from jax.experimental.pallas import tpu as pltpu
from jax.sharding import Mesh
from jax.sharding import PartitionSpec as P

SEQ = ("seq_0", "seq_1")
DP = ("dp_0", "dp_1")

C = 192
TXT = 384
FR = 1536
OWN = 32
GRP = 256
TB = TXT // OWN
FB = FR // OWN
NU = 4
NCH = GRP // OWN // NU
ROWS = (NU + NU // 2) * FB
PROWS = (GRP // OWN) * 3 // 2 * TB
CUT = 224
LONG = FR - FR // 4
PAD = 296
KP = 2 * 3 * 128
FRAME_UNROLL = 16
TOKEN_UNROLL = 6
NN = TB * 128
MB = 384

HALF_LOG_TWO_PI = 0.9189385332046727
NEG = -2.0e11
F32 = jnp.float32
BF16 = jnp.bfloat16
NT = (((1,), (1,)), ((), ()))
NN_DIMS = (((1,), (0,)), ((), ()))


def call(body, out_shape, n_in, scratch=(), smem=(), hbm=(), mib=24):
    vmem = pl.BlockSpec(memory_space=pltpu.VMEM)
    return pl.pallas_call(
        body,
        out_shape=out_shape,
        in_specs=[
            pl.BlockSpec(memory_space=pltpu.SMEM if i in smem else pl.ANY if i in hbm else pltpu.VMEM)
            for i in range(n_in)
        ],
        out_specs=jax.tree.map(lambda _: vmem, out_shape),
        scratch_shapes=list(scratch),
        compiler_params=pltpu.CompilerParams(vmem_limit_bytes=mib * 1024 * 1024),
    )


def one_hot(rank_row, first, count, dtype):
    ids = lax.broadcasted_iota(jnp.int32, (count, GRP), 0) + first
    return jnp.where(ids == rank_row, 1.0, 0.0).astype(dtype)


def pack_block(x, picks, stage, at, pair_at, step, count):
    got = lax.dot_general(picks, x, NT, preferred_element_type=F32)
    for k in range(count):
        stage[pl.ds(at + k * step, OWN, stride=PAD), :] = got[k * OWN : (k + 1) * OWN, 0:128]
    for p in range(count // 2):
        low = got[2 * p * OWN : (2 * p + 1) * OWN, 128:C]
        high = got[(2 * p + 1) * OWN : (2 * p + 2) * OWN, 128:C]
        stage[pl.ds(pair_at + p * step, OWN, stride=PAD), :] = jnp.concatenate([low, high], axis=1)


def stage_priors(rank_ref, means_ref, logs_ref, stage):
    picks = one_hot(rank_ref[...], 0, GRP, BF16)
    count = GRP // OWN

    def tokens(i, _):
        for q in range(TOKEN_UNROLL):
            for which, ref in enumerate((means_ref, logs_ref)):
                token = i * TOKEN_UNROLL + q
                at = which * PROWS + token
                pack_block(ref[token], picks, stage, at, at + count * TB, TB, count)
        return 0

    lax.fori_loop(0, TB // TOKEN_UNROLL, tokens, 0)


def stage_latents(chunk, rank_ref, lat_ref, stage):
    picks = one_hot(rank_ref[...], chunk * NU * OWN, NU * OWN, BF16)

    def frames(j, _):
        for q in range(FRAME_UNROLL):
            frame = j * FRAME_UNROLL + q
            pack_block(lat_ref[frame], picks, stage, frame, frame + NU * FB, FB, NU)
        return 0

    lax.fori_loop(0, FB // FRAME_UNROLL, frames, 0)


def unstage(stage, out_ref, first, rows):
    for d in range(OWN):
        out_ref[d, first : first + rows, :] = stage[d * PAD : d * PAD + rows, :].astype(BF16)


def pack_first(rank_ref, means_ref, logs_ref, lat_ref, out_ref, stage):
    stage_priors(rank_ref, means_ref, logs_ref, stage)
    unstage(stage, out_ref, 0, 2 * PROWS)
    stage_latents(0, rank_ref, lat_ref, stage)
    unstage(stage, out_ref, 2 * PROWS, ROWS)


def pack_second(rank_ref, lat_ref, out_ref, stage):
    stage_latents(1, rank_ref, lat_ref, stage)
    unstage(stage, out_ref, 0, ROWS)


def build_sides(y_ref, text_ref, rhs0_ref, rhs1_ref, bias0_ref, bias1_ref, wt, pr, zz, zs):
    wide = 152
    for s in range(OWN):
        m = y_ref[s, 0:PROWS, :].astype(F32)
        ls = y_ref[s, PROWS : 2 * PROWS, :].astype(F32)
        prec = jnp.exp(-2.0 * ls)
        wt[s * wide : s * wide + PROWS, :] = m * prec
        pr[s * wide : s * wide + PROWS, :] = prec
        zz[s * wide : s * wide + PROWS, :] = 0.5 * (m * m * prec) + ls
    lane = lax.broadcasted_iota(jnp.int32, (OWN, 128), 1)
    none = jnp.zeros((OWN, 128), F32)
    ones = jnp.ones((8, 128), F32)
    lane8 = lax.broadcasted_iota(jnp.int32, (8, 128), 1)
    count = GRP // OWN

    def rows_of(ref, block, i):
        return ref[pl.ds(block * TB + i, OWN, stride=wide), :]

    def both(ref, pair, i):
        x = rows_of(ref, count + pair, i)
        return [jnp.where(lane < 64, x, 0.0), jnp.where(lane >= 64, x, 0.0)]

    for pair in range(count // 2):
        c, p = pair // 2, pair % 2
        for v in range(TB // 2):
            for half, (ref, factor) in enumerate(((wt, 1.0), (pr, -0.5))):
                first, second, mixed = [], [], []
                for i in (2 * v, 2 * v + 1):
                    first += [rows_of(ref, 2 * pair, i), none]
                    second += [none, rows_of(ref, 2 * pair + 1, i)]
                    mixed += both(ref, pair, i)
                for q, pieces in enumerate((first, second, mixed)):
                    turned = jnp.concatenate(pieces, axis=0).T.astype(BF16)
                    k = (half * 3 + q) * 128
                    (rhs0_ref, rhs1_ref)[c][p, k : k + 128, v * 128 : (v + 1) * 128] = turned * jnp.asarray(factor, BF16)
        for i in range(TB):
            for k, extra in enumerate(both(zz, pair, i)):
                at = c * NN + i * 128 + (2 * p + k) * OWN
                zs[at : at + OWN, :] = rows_of(zz, 2 * pair + k, i) + extra
    for c in range(NCH):
        text = text_ref[c]
        for i in range(TB):
            total = lax.dot_general(
                ones,
                zs[c * NN + i * 128 : c * NN + (i + 1) * 128, :],
                NT,
                precision=lax.Precision.HIGHEST,
                preferred_element_type=F32,
            )
            token = (lane8 % OWN) * TB + i
            (bias0_ref, bias1_ref)[c][:, i * 128 : (i + 1) * 128] = jnp.where(
                token < text, -total - C * HALF_LOG_TWO_PI, NEG
            )


def search(chunk, first_row, count_ref, y_ref, rhs_ref, bias_ref, text_ref, frame_ref, *rest):
    if chunk == 0:
        out_ref, lhs, lik, buf0, buf1 = rest
        out_ref[...] = jnp.zeros(out_ref.shape, F32)
    else:
        earlier_ref, far_ref, out_ref, lhs, lik, buf0, buf1, far, sem = rest
        out_ref[...] = earlier_ref[...]
    per = MB // FB
    wide_lane = lax.broadcasted_iota(jnp.int32, (MB, 128), 1)

    def pieces_of(b, q, k):
        if chunk == 0:
            return ((y_ref, b * per + q, first_row + k * FB, FB),)
        own = max(0, min(FB, CUT - k * FB))
        parts = ((y_ref, b * per + q, k * FB, own),)
        rest = pl.multiple_of(b * (ROWS - CUT) + (k * FB + own - CUT), 16) if own < FB else 0
        return parts + ((y_ref, 3 * per + q, rest, FB - own),)

    def far_pieces(b, q, k):
        return ((far, q, k * FB, FB),)

    def matmul_block(b, _, pieces=pieces_of):
        for q in range(per):
            for p in range(NU // 2):
                for n, k in enumerate((2 * p, 2 * p + 1, NU + p)):
                    at = p * KP + n * 128
                    done = q * FB
                    for ref, s, row, rows in pieces(b, q, k):
                        if not rows:
                            continue
                        x = ref[s, pl.ds(row, rows), :]
                        lhs[done : done + rows, at : at + 128] = x
                        wide = x.astype(F32)
                        lhs[done : done + rows, at + 384 : at + 512] = (wide * wide).astype(BF16)
                        done += rows
        group = pl.ds(b * (MB // 8), MB // 8)
        for t in range(KP // 256):
            got = [
                lax.dot_general(
                    lhs[:, p * KP : (p + 1) * KP],
                    rhs_ref[p, :, t * 256 : (t + 1) * 256],
                    NN_DIMS,
                    preferred_element_type=F32,
                )
                for p in range(2)
            ]
            for h in range(2):
                one, two = (g[:, h * 128 : (h + 1) * 128] for g in got)
                i = 4 * t + 2 * h
                even = jnp.where(wide_lane < 64, one, pltpu.roll(two, 64, 1))
                odd = jnp.where(wide_lane < 64, pltpu.roll(one, 64, 1), two)
                for n, x in enumerate((even, odd)):
                    cols = slice((i + n) * 128, (i + n + 1) * 128)
                    lik[group, :, cols] = (x + bias_ref[0:1, cols]).reshape(MB // 8, 8, 128)
        return 0

    if chunk == 0:
        lax.fori_loop(0, count_ref[chunk], matmul_block, 0)
    else:
        lax.fori_loop(0, jnp.minimum(count_ref[chunk], 3), matmul_block, 0)

        @pl.when(count_ref[chunk] > 3)
        def _():
            copy = pltpu.make_async_copy(far_ref, far, sem)
            copy.start()
            copy.wait()
            matmul_block(3, 0, far_pieces)

    lane = lax.broadcasted_iota(jnp.int32, (8, 128), 1)
    sub = lax.broadcasted_iota(jnp.int32, (8, 128), 0)
    block = lane % OWN
    seg = lane // OWN
    lane1 = lax.broadcasted_iota(jnp.int32, (1, 128), 1)
    first1 = (lane1 % OWN) == 0
    block_start = (block * TB).astype(F32)
    text = text_ref[chunk]
    frames = frame_ref[chunk]
    base = block * TB + frames - text
    inverse = 1.0 / (text - 1).astype(F32)
    scale = math.log2(math.e) / C

    def run_frames(at, state, buf, opening):
        for j in range(FB):
            entering = jnp.where(first1, opening if j == 0 else NEG, pltpu.roll(state[TB - 1], 1, 1))
            new = []
            for i in range(TB):
                like = lik[at + j // 8, j % 8 : j % 8 + 1, i * 128 : (i + 1) * 128]
                before = entering if i == 0 else state[i - 1]
                now = like + jnp.maximum(state[i], before)
                buf[j : j + 1, i * 128 : (i + 1) * 128] = now
                new.append(now)
            state = new
        return state

    def by_segment(x, reduce, fill):
        out = None
        for k in range(NU):
            one = reduce(jnp.where(seg == k, x, fill), axis=1, keepdims=True)
            out = jnp.broadcast_to(one, (8, 128)) if out is None else jnp.where(seg == k, one, out)
        return out

    seg_rows = lax.broadcasted_iota(jnp.int32, (128, 128), 0) // OWN
    seg_cols = lax.broadcasted_iota(jnp.int32, (128, 128), 1) // OWN
    same = jnp.where(seg_rows == seg_cols, 1.0, 0.0).astype(BF16)

    def over_segment(x):
        high = x.astype(BF16)
        rest = x - high.astype(F32)
        mid = rest.astype(BF16)
        low = (rest - mid.astype(F32)).astype(BF16)
        parts = [lax.dot_general(y, same, NN_DIMS, preferred_element_type=F32) for y in (high, mid, low)]
        return parts[0] + (parts[1] + parts[2])

    def soften(index, buf, finish):
        frame = index * FB + lax.broadcasted_iota(jnp.int32, (FB, 128), 0)
        weights, moments, tops = [], [], []
        for g in range(FB // 8):
            late = index * FB + g * 8 + sub - base
            xs = [
                jnp.where(late <= i, buf[g * 8 : (g + 1) * 8, i * 128 : (i + 1) * 128], 8 * NEG)
                for i in range(TB)
            ]
            top = by_segment(functools.reduce(jnp.maximum, xs), jnp.max, -3.0e38)
            ws = [jnp.exp2((x - top) * scale) for x in xs]
            suffix = ws[TB - 1]
            moment = suffix
            for i in range(TB - 2, 0, -1):
                suffix = suffix + ws[i]
                moment = moment + suffix
            weight = suffix + ws[0]
            weights.append(weight)
            moments.append(moment + block_start * weight)
            tops.append(top)
        weight, moment = (over_segment(jnp.concatenate(x, axis=0)) for x in (weights, moments))
        place = jnp.where(frame < frames[0:1], moment / weight * inverse[0:1], 0.0)
        ended = jnp.where(frame == frames[0:1] - 1, jnp.concatenate(tops, axis=0), 0.0)
        finish = finish + jnp.sum(ended.reshape(FB // 8, 8, 128), axis=0)
        rows = [place]
        turned = jnp.concatenate(rows + [jnp.zeros((128 - FB, 128), F32)], axis=0).T
        where = jnp.maximum(index, 0)
        for k in range(NU):
            out_ref[where, chunk * NU + k : chunk * NU + k + 1, :] = turned[k * OWN : k * OWN + 1, :]
        return finish

    def pair(b, carried):
        state, finish = list(carried[:TB]), carried[TB]
        state = run_frames(b * (2 * FB // 8), state, buf0, jnp.where(b == 0, 0.0, NEG))
        finish = soften(2 * b - 1, buf1, finish)
        state = run_frames(b * (2 * FB // 8) + FB // 8, state, buf1, NEG)
        finish = soften(2 * b, buf0, finish)
        return (*state, finish)

    start = [jnp.full((1, 128), NEG, F32) for _ in range(TB)]
    carried = lax.fori_loop(0, count_ref[NCH + chunk], pair, (*start, jnp.zeros((8, 128), F32)))
    finish = soften(2 * count_ref[NCH + chunk] - 1, buf1, carried[TB])
    finish = jnp.sum(finish, axis=0, keepdims=True) * (1.0 / C)
    finish = jnp.sum(jnp.where(first1, finish, 0.0), axis=1, keepdims=True)
    for d in range(OWN):
        out_ref[d, chunk * NU : chunk * NU + 1, 64:128] = jnp.broadcast_to(finish, (1, 64))


def unpack(rank_ref, got_ref, pos_ref, turned):
    rows = [got_ref[pl.ds(k, OWN, stride=8), :] for k in range(NCH * NU)]
    for c in range(2):
        turned[:, c * 128 : (c + 1) * 128] = jnp.concatenate(rows[c * 4 : c * 4 + 4], axis=0).T
    picks = one_hot(rank_ref[...], 0, GRP, F32)
    pos_ref[...] = lax.dot_general(
        turned[0:FB, :], picks, NN_DIMS, precision=lax.Precision.HIGHEST, preferred_element_type=F32
    )


def sum_up(back, frame_lens):
    finish = jnp.sum(back, axis=(0, 1), keepdims=True)[0]
    lens = jnp.sum(frame_lens).astype(F32)
    lanes = lax.broadcasted_iota(jnp.int32, (1, 128), 1)
    return jnp.where(lanes >= 64, finish, lens)


def exchange(x):
    return lax.all_to_all(x, SEQ, split_axis=0, concat_axis=0, tiled=True)


def over_dp(x, combine):
    x = combine(x, lax.ppermute(x, "dp_1", [(0, 1), (1, 0)]))
    for n in (1, 2):
        x = combine(x, lax.ppermute(x, "dp_0", [(i, (i + n) % 4) for i in range(4)]))
    return x


def exchange_short(first, x, rank, frame_lens):
    relayed = [lax.ppermute(x[:, CUT:], "seq_0", [(i, 3)]) for i in range(3)]
    relayed = jnp.concatenate([*relayed, x[:, : CUT - 3 * (ROWS - CUT)]], axis=1)
    send = jnp.where(lax.axis_index("seq_0") == 3, relayed, x[:, :CUT])
    first, send = lax.optimization_barrier((first, send))
    got = exchange(send)
    longest = jnp.max(jnp.where(rank[0] >= NU * OWN, frame_lens, 0)).astype(F32)
    longest = over_dp(jnp.full((1, 128), longest), jnp.maximum)[0, 0]
    last = slice(3 * OWN // 4, OWN)
    got, longest = lax.optimization_barrier((got, longest))
    none = lambda v: jnp.zeros((OWN // 4, ROWS, 128), BF16)
    far = lax.cond(longest > LONG, lambda v: exchange(v)[last], none, x)
    return first, got, far


def make_rhs(first, text_lanes):
    wide = pltpu.VMEM((OWN * 152, 128), F32)
    return call(
        build_sides,
        (jax.ShapeDtypeStruct((2, KP, KP), BF16),) * NCH + (jax.ShapeDtypeStruct((8, NN), F32),) * NCH,
        2,
        (wide, wide, wide, pltpu.VMEM((NCH * NN, 128), F32)),
        mib=32,
    )(first, text_lanes)


def run_search(chunk, first_row, *operands):
    more = (pltpu.VMEM((OWN // 4, ROWS, 128), BF16), pltpu.SemaphoreType.DMA) if chunk else ()
    return call(
        functools.partial(search, chunk, first_row),
        jax.ShapeDtypeStruct((OWN, 8, 128), F32),
        len(operands),
        (
            pltpu.VMEM((MB, 2 * KP), BF16),
            pltpu.VMEM((FR // 8, 8, NN), F32),
            pltpu.VMEM((FB, NN), F32),
            pltpu.VMEM((FB, NN), F32),
            *more,
        ),
        smem=(0,),
        hbm=(7,) if chunk else (),
    )(*operands)


def pack_call(body, rows, *operands):
    return call(
        body,
        jax.ShapeDtypeStruct((OWN, rows, 128), BF16),
        len(operands),
        (pltpu.VMEM((OWN * PAD, 128), F32),),
    )(*operands)


def ranks(frame_lens):
    ids = jnp.arange(GRP, dtype=jnp.int32)
    a, b = frame_lens[:, None], frame_lens[None, :]
    ahead = (a > b) | ((a == b) & (ids[:, None] < ids[None, :]))
    return jnp.sum(ahead.astype(jnp.int32), axis=0)[None, :]


def owned(lens, rank, own):
    slots = jnp.arange(GRP // OWN, dtype=jnp.int32) * OWN + own
    return jnp.sum(jnp.where(rank == slots[:, None], lens[None, :], 0), axis=1)


def lanes_of(lens):
    parts = jnp.repeat(lens.reshape(NCH, 1, NU), OWN, axis=2)
    return jnp.broadcast_to(parts, (NCH, 8, 128))


def counts_of(frame_own):
    longest = jnp.max(frame_own.reshape(NCH, NU), axis=1)
    return jnp.concatenate([(longest + MB - 1) // MB, (longest + 2 * FB - 1) // (2 * FB)])


def shards(means, log_scales, latents, text_lens, frame_lens):
    own = lax.axis_index(SEQ).astype(jnp.int32)
    rank = ranks(frame_lens)
    text_own, frame_own = owned(text_lens, rank, own), owned(frame_lens, rank, own)
    means, log_scales, latents = (jnp.transpose(x, (1, 2, 0)) for x in (means, log_scales, latents))
    packed = pack_call(pack_first, 2 * PROWS + ROWS, rank, means, log_scales, latents)
    packed, later_rank, latents, later_lens = lax.optimization_barrier((packed, rank, latents, frame_lens))
    first = exchange(packed)
    packed = pack_call(pack_second, ROWS, later_rank, latents)
    first, second, far = exchange_short(first, packed, later_rank, later_lens)
    text_lanes, frame_lanes, counts = lanes_of(text_own), lanes_of(frame_own), counts_of(frame_own)
    rhs0, rhs1, bias0, bias1 = make_rhs(first, text_lanes)
    back = run_search(0, 2 * PROWS, counts, first, rhs0, bias0, text_lanes, frame_lanes)
    back = exchange(run_search(1, 0, counts, second, rhs1, bias1, text_lanes, frame_lanes, back, far))
    sums = over_dp(sum_up(back, frame_lens), jnp.add)
    pos = call(
        unpack, jax.ShapeDtypeStruct((FB, GRP), F32), 2, (pltpu.VMEM((128, 2 * 128), F32),)
    )(rank, back.reshape(OWN * 8, 128))
    return (jnp.transpose(pos), -sums[0, 64] / sums[0, 0])


def solution(mesh):
    torus = Mesh(mesh.devices.reshape(4, 2, 4, 8), ("dp_0", "dp_1", "seq_0", "seq_1"))
    in_specs = (P(DP, SEQ, None), P(DP, SEQ, None), P(DP, SEQ, None), P(DP), P(DP))
    out_specs = (P(DP, SEQ), P())
    return jax.shard_map(
        shards, mesh=torus, in_specs=in_specs, out_specs=out_specs, check_vma=False
    )
```

```python
import functools
import math

import jax
import jax.numpy as jnp
from jax import lax
from jax.experimental import pallas as pl
from jax.experimental.pallas import tpu as pltpu
from jax.sharding import Mesh
from jax.sharding import PartitionSpec as P

SEQ = ("seq_0", "seq_1")
DP = ("dp_0", "dp_1")

C = 192
TXT = 384
FR = 1536
OWN = 32
GRP = 256
TB = TXT // OWN
FB = FR // OWN
NU = 4
NCH = GRP // OWN // NU
ROWS = (NU + NU // 2) * FB
PROWS = (GRP // OWN) * 3 // 2 * TB
CUT = 224
LONG = FR - FR // 4
PAD = 296
KP = 2 * 3 * 128
FRAME_UNROLL = 16
TOKEN_UNROLL = 6
NN = TB * 128
MB = 384

HALF_LOG_TWO_PI = 0.9189385332046727
NEG = -2.0e11
F32 = jnp.float32
BF16 = jnp.bfloat16
NT = (((1,), (1,)), ((), ()))
NN_DIMS = (((1,), (0,)), ((), ()))


def call(body, out_shape, n_in, scratch=(), smem=(), hbm=(), mib=24):
    vmem = pl.BlockSpec(memory_space=pltpu.VMEM)
    return pl.pallas_call(
        body,
        out_shape=out_shape,
        in_specs=[
            pl.BlockSpec(memory_space=pltpu.SMEM if i in smem else pl.ANY if i in hbm else pltpu.VMEM)
            for i in range(n_in)
        ],
        out_specs=jax.tree.map(lambda _: vmem, out_shape),
        scratch_shapes=list(scratch),
        compiler_params=pltpu.CompilerParams(vmem_limit_bytes=mib * 1024 * 1024),
    )


def one_hot(rank_row, first, count, dtype):
    ids = lax.broadcasted_iota(jnp.int32, (count, GRP), 0) + first
    return jnp.where(ids == rank_row, 1.0, 0.0).astype(dtype)


def pack_block(x, picks, stage, at, pair_at, step, count):
    got = lax.dot_general(picks, x, NT, preferred_element_type=F32)
    for k in range(count):
        stage[pl.ds(at + k * step, OWN, stride=PAD), :] = got[k * OWN : (k + 1) * OWN, 0:128]
    for p in range(count // 2):
        low = got[2 * p * OWN : (2 * p + 1) * OWN, 128:C]
        high = got[(2 * p + 1) * OWN : (2 * p + 2) * OWN, 128:C]
        stage[pl.ds(pair_at + p * step, OWN, stride=PAD), :] = jnp.concatenate([low, high], axis=1)


def stage_priors(rank_ref, means_ref, logs_ref, stage):
    picks = one_hot(rank_ref[...], 0, GRP, BF16)
    count = GRP // OWN

    def tokens(i, _):
        for q in range(TOKEN_UNROLL):
            for which, ref in enumerate((means_ref, logs_ref)):
                token = i * TOKEN_UNROLL + q
                at = which * PROWS + token
                pack_block(ref[token], picks, stage, at, at + count * TB, TB, count)
        return 0

    lax.fori_loop(0, TB // TOKEN_UNROLL, tokens, 0)


def stage_latents(chunk, rank_ref, lat_ref, stage, ready=None):
    picks = one_hot(rank_ref[...], chunk * NU * OWN, NU * OWN, BF16)

    def frames(j, _):
        if ready:
            ready(j)
        for q in range(FRAME_UNROLL):
            frame = j * FRAME_UNROLL + q
            pack_block(lat_ref[frame], picks, stage, frame, frame + NU * FB, FB, NU)
        return 0

    lax.fori_loop(0, FB // FRAME_UNROLL, frames, 0)


def unstage(stage, out_ref, first, rows):
    for d in range(OWN):
        out_ref[d, first : first + rows, :] = stage[d * PAD : d * PAD + rows, :].astype(BF16)


def pack_first(rank_ref, means_hbm, logs_hbm, lat_hbm, out_hbm, stage, means, logs, lat, out0, out1, sems):
    def piece(j):
        part = pl.ds(j * FRAME_UNROLL, FRAME_UNROLL)
        return pltpu.make_async_copy(lat_hbm.at[part], lat.at[part], sems.at[4 + j])

    priors = [
        pltpu.make_async_copy(means_hbm, means, sems.at[0]),
        pltpu.make_async_copy(logs_hbm, logs, sems.at[1]),
    ]
    outs = [
        pltpu.make_async_copy(out0, out_hbm.at[:, pl.ds(0, 2 * PROWS)], sems.at[2]),
        pltpu.make_async_copy(out1, out_hbm.at[:, pl.ds(2 * PROWS, ROWS)], sems.at[3]),
    ]
    for copy in (*priors, *(piece(j) for j in range(FB // FRAME_UNROLL))):
        copy.start()
    for copy in priors:
        copy.wait()
    stage_priors(rank_ref, means, logs, stage)
    unstage(stage, out0, 0, 2 * PROWS)
    outs[0].start()
    stage_latents(0, rank_ref, lat, stage, lambda j: piece(j).wait())
    unstage(stage, out1, 0, ROWS)
    outs[1].start()
    for copy in outs:
        copy.wait()


def pack_whole(rank, means, log_scales, latents):
    hbm, vmem = pl.BlockSpec(memory_space=pltpu.HBM), pl.BlockSpec(memory_space=pltpu.VMEM)
    half = pltpu.VMEM((OWN, ROWS, 128), BF16)
    return pl.pallas_call(
        pack_first,
        out_shape=jax.ShapeDtypeStruct((OWN, 2 * PROWS + ROWS, 128), BF16),
        in_specs=[vmem, hbm, hbm, hbm],
        out_specs=hbm,
        scratch_shapes=[
            pltpu.VMEM((OWN * PAD, 128), F32),
            *(pltpu.VMEM(x.shape, BF16) for x in (means, log_scales, latents)),
            half,
            half,
            pltpu.SemaphoreType.DMA((4 + FB // FRAME_UNROLL,)),
        ],
        compiler_params=pltpu.CompilerParams(vmem_limit_bytes=63 * 1024 * 1024),
    )(rank, means, log_scales, latents)


def pack_second(rank_ref, lat_ref, out_ref, stage):
    stage_latents(1, rank_ref, lat_ref, stage)
    unstage(stage, out_ref, 0, ROWS)


def build_sides(y_ref, text_ref, rhs0_ref, rhs1_ref, bias0_ref, bias1_ref, wt, pr, zz, zs):
    wide = 152
    for s in range(OWN):
        m = y_ref[s, 0:PROWS, :].astype(F32)
        ls = y_ref[s, PROWS : 2 * PROWS, :].astype(F32)
        prec = jnp.exp(-2.0 * ls)
        wt[s * wide : s * wide + PROWS, :] = m * prec
        pr[s * wide : s * wide + PROWS, :] = prec
        zz[s * wide : s * wide + PROWS, :] = 0.5 * (m * m * prec) + ls
    lane = lax.broadcasted_iota(jnp.int32, (OWN, 128), 1)
    none = jnp.zeros((OWN, 128), F32)
    ones = jnp.ones((8, 128), F32)
    lane8 = lax.broadcasted_iota(jnp.int32, (8, 128), 1)
    count = GRP // OWN

    def rows_of(ref, block, i):
        return ref[pl.ds(block * TB + i, OWN, stride=wide), :]

    def both(ref, pair, i):
        x = rows_of(ref, count + pair, i)
        return [jnp.where(lane < 64, x, 0.0), jnp.where(lane >= 64, x, 0.0)]

    for pair in range(count // 2):
        c, p = pair // 2, pair % 2
        for v in range(TB // 2):
            for half, (ref, factor) in enumerate(((wt, 1.0), (pr, -0.5))):
                first, second, mixed = [], [], []
                for i in (2 * v, 2 * v + 1):
                    first += [rows_of(ref, 2 * pair, i), none]
                    second += [none, rows_of(ref, 2 * pair + 1, i)]
                    mixed += both(ref, pair, i)
                for q, pieces in enumerate((first, second, mixed)):
                    turned = jnp.concatenate(pieces, axis=0).T.astype(BF16)
                    k = (half * 3 + q) * 128
                    (rhs0_ref, rhs1_ref)[c][p, k : k + 128, v * 128 : (v + 1) * 128] = turned * jnp.asarray(factor, BF16)
        for i in range(TB):
            for k, extra in enumerate(both(zz, pair, i)):
                at = c * NN + i * 128 + (2 * p + k) * OWN
                zs[at : at + OWN, :] = rows_of(zz, 2 * pair + k, i) + extra
    for c in range(NCH):
        text = text_ref[c]
        for i in range(TB):
            total = lax.dot_general(
                ones,
                zs[c * NN + i * 128 : c * NN + (i + 1) * 128, :],
                NT,
                precision=lax.Precision.HIGHEST,
                preferred_element_type=F32,
            )
            token = (lane8 % OWN) * TB + i
            (bias0_ref, bias1_ref)[c][:, i * 128 : (i + 1) * 128] = jnp.where(
                token < text, -total - C * HALF_LOG_TWO_PI, NEG
            )


def search(chunk, first_row, count_ref, y_ref, rhs_ref, bias_ref, text_ref, frame_ref, *rest):
    if chunk == 0:
        out_ref, lhs, lik, buf0, buf1 = rest
        out_ref[...] = jnp.zeros(out_ref.shape, F32)
    else:
        earlier_ref, far_ref, out_ref, lhs, lik, buf0, buf1, far, sem = rest
        out_ref[...] = earlier_ref[...]
    per = MB // FB
    wide_lane = lax.broadcasted_iota(jnp.int32, (MB, 128), 1)

    def pieces_of(b, q, k):
        if chunk == 0:
            return ((y_ref, b * per + q, first_row + k * FB, FB),)
        own = max(0, min(FB, CUT - k * FB))
        parts = ((y_ref, b * per + q, k * FB, own),)
        rest = pl.multiple_of(b * (ROWS - CUT) + (k * FB + own - CUT), 16) if own < FB else 0
        return parts + ((y_ref, 3 * per + q, rest, FB - own),)

    def far_pieces(b, q, k):
        return ((far, q, k * FB, FB),)

    def matmul_block(b, _, pieces=pieces_of):
        for q in range(per):
            for p in range(NU // 2):
                for n, k in enumerate((2 * p, 2 * p + 1, NU + p)):
                    at = p * KP + n * 128
                    done = q * FB
                    for ref, s, row, rows in pieces(b, q, k):
                        if not rows:
                            continue
                        x = ref[s, pl.ds(row, rows), :]
                        lhs[done : done + rows, at : at + 128] = x
                        wide = x.astype(F32)
                        lhs[done : done + rows, at + 384 : at + 512] = (wide * wide).astype(BF16)
                        done += rows
        group = pl.ds(b * (MB // 8), MB // 8)
        for t in range(KP // 256):
            got = [
                lax.dot_general(
                    lhs[:, p * KP : (p + 1) * KP],
                    rhs_ref[p, :, t * 256 : (t + 1) * 256],
                    NN_DIMS,
                    preferred_element_type=F32,
                )
                for p in range(2)
            ]
            for h in range(2):
                one, two = (g[:, h * 128 : (h + 1) * 128] for g in got)
                i = 4 * t + 2 * h
                even = jnp.where(wide_lane < 64, one, pltpu.roll(two, 64, 1))
                odd = jnp.where(wide_lane < 64, pltpu.roll(one, 64, 1), two)
                for n, x in enumerate((even, odd)):
                    cols = slice((i + n) * 128, (i + n + 1) * 128)
                    lik[group, :, cols] = (x + bias_ref[0:1, cols]).reshape(MB // 8, 8, 128)
        return 0

    if chunk == 0:
        lax.fori_loop(0, count_ref[chunk], matmul_block, 0)
    else:
        lax.fori_loop(0, jnp.minimum(count_ref[chunk], 3), matmul_block, 0)

        @pl.when(count_ref[chunk] > 3)
        def _():
            copy = pltpu.make_async_copy(far_ref, far, sem)
            copy.start()
            copy.wait()
            matmul_block(3, 0, far_pieces)

    lane = lax.broadcasted_iota(jnp.int32, (8, 128), 1)
    sub = lax.broadcasted_iota(jnp.int32, (8, 128), 0)
    block = lane % OWN
    seg = lane // OWN
    lane1 = lax.broadcasted_iota(jnp.int32, (1, 128), 1)
    first1 = (lane1 % OWN) == 0
    block_start = (block * TB).astype(F32)
    text = text_ref[chunk]
    frames = frame_ref[chunk]
    base = block * TB + frames - text
    inverse = 1.0 / (text - 1).astype(F32)
    scale = math.log2(math.e) / C

    def run_frames(at, state, buf, opening):
        for j in range(FB):
            entering = jnp.where(first1, opening if j == 0 else NEG, pltpu.roll(state[TB - 1], 1, 1))
            new = []
            for i in range(TB):
                like = lik[at + j // 8, j % 8 : j % 8 + 1, i * 128 : (i + 1) * 128]
                before = entering if i == 0 else state[i - 1]
                now = like + jnp.maximum(state[i], before)
                buf[j : j + 1, i * 128 : (i + 1) * 128] = now
                new.append(now)
            state = new
        return state

    def by_segment(x, reduce, fill):
        out = None
        for k in range(NU):
            one = reduce(jnp.where(seg == k, x, fill), axis=1, keepdims=True)
            out = jnp.broadcast_to(one, (8, 128)) if out is None else jnp.where(seg == k, one, out)
        return out

    seg_rows = lax.broadcasted_iota(jnp.int32, (128, 128), 0) // OWN
    seg_cols = lax.broadcasted_iota(jnp.int32, (128, 128), 1) // OWN
    same = jnp.where(seg_rows == seg_cols, 1.0, 0.0).astype(BF16)

    def over_segment(x):
        high = x.astype(BF16)
        rest = x - high.astype(F32)
        mid = rest.astype(BF16)
        low = (rest - mid.astype(F32)).astype(BF16)
        parts = [lax.dot_general(y, same, NN_DIMS, preferred_element_type=F32) for y in (high, mid, low)]
        return parts[0] + (parts[1] + parts[2])

    def soften(index, buf, finish):
        frame = index * FB + lax.broadcasted_iota(jnp.int32, (FB, 128), 0)
        weights, moments, tops = [], [], []
        for g in range(FB // 8):
            late = index * FB + g * 8 + sub - base
            xs = [
                jnp.where(late <= i, buf[g * 8 : (g + 1) * 8, i * 128 : (i + 1) * 128], 8 * NEG)
                for i in range(TB)
            ]
            top = by_segment(functools.reduce(jnp.maximum, xs), jnp.max, -3.0e38)
            ws = [jnp.exp2((x - top) * scale) for x in xs]
            suffix = ws[TB - 1]
            moment = suffix
            for i in range(TB - 2, 0, -1):
                suffix = suffix + ws[i]
                moment = moment + suffix
            weight = suffix + ws[0]
            weights.append(weight)
            moments.append(moment + block_start * weight)
            tops.append(top)
        weight, moment = (over_segment(jnp.concatenate(x, axis=0)) for x in (weights, moments))
        place = jnp.where(frame < frames[0:1], moment / weight * inverse[0:1], 0.0)
        ended = jnp.where(frame == frames[0:1] - 1, jnp.concatenate(tops, axis=0), 0.0)
        finish = finish + jnp.sum(ended.reshape(FB // 8, 8, 128), axis=0)
        rows = [place]
        turned = jnp.concatenate(rows + [jnp.zeros((128 - FB, 128), F32)], axis=0).T
        where = jnp.maximum(index, 0)
        for k in range(NU):
            out_ref[where, chunk * NU + k : chunk * NU + k + 1, :] = turned[k * OWN : k * OWN + 1, :]
        return finish

    def pair(b, carried):
        state, finish = list(carried[:TB]), carried[TB]
        state = run_frames(b * (2 * FB // 8), state, buf0, jnp.where(b == 0, 0.0, NEG))
        finish = soften(2 * b - 1, buf1, finish)
        state = run_frames(b * (2 * FB // 8) + FB // 8, state, buf1, NEG)
        finish = soften(2 * b, buf0, finish)
        return (*state, finish)

    start = [jnp.full((1, 128), NEG, F32) for _ in range(TB)]
    carried = lax.fori_loop(0, count_ref[NCH + chunk], pair, (*start, jnp.zeros((8, 128), F32)))
    finish = soften(2 * count_ref[NCH + chunk] - 1, buf1, carried[TB])
    finish = jnp.sum(finish, axis=0, keepdims=True) * (1.0 / C)
    finish = jnp.sum(jnp.where(first1, finish, 0.0), axis=1, keepdims=True)
    for d in range(OWN):
        out_ref[d, chunk * NU : chunk * NU + 1, 64:128] = jnp.broadcast_to(finish, (1, 64))


def unpack(rank_ref, got_ref, pos_ref, turned):
    rows = [got_ref[pl.ds(k, OWN, stride=8), :] for k in range(NCH * NU)]
    for c in range(2):
        turned[:, c * 128 : (c + 1) * 128] = jnp.concatenate(rows[c * 4 : c * 4 + 4], axis=0).T
    picks = one_hot(rank_ref[...], 0, GRP, F32)
    pos_ref[...] = lax.dot_general(
        turned[0:FB, :], picks, NN_DIMS, precision=lax.Precision.HIGHEST, preferred_element_type=F32
    )


def sum_up(back, frame_lens):
    finish = jnp.sum(back, axis=(0, 1), keepdims=True)[0]
    lens = jnp.sum(frame_lens).astype(F32)
    lanes = lax.broadcasted_iota(jnp.int32, (1, 128), 1)
    return jnp.where(lanes >= 64, finish, lens)


def exchange(x):
    return lax.all_to_all(x, SEQ, split_axis=0, concat_axis=0, tiled=True)


def over_dp(x, combine):
    x = combine(x, lax.ppermute(x, "dp_1", [(0, 1), (1, 0)]))
    for n in (1, 2):
        x = combine(x, lax.ppermute(x, "dp_0", [(i, (i + n) % 4) for i in range(4)]))
    return x


def exchange_short(first, x, rank, frame_lens):
    relayed = [lax.ppermute(x[:, CUT:], "seq_0", [(i, 3)]) for i in range(3)]
    relayed = jnp.concatenate([*relayed, x[:, : CUT - 3 * (ROWS - CUT)]], axis=1)
    send = jnp.where(lax.axis_index("seq_0") == 3, relayed, x[:, :CUT])
    longest = jnp.max(jnp.where(rank[0] >= NU * OWN, frame_lens, 0)).astype(F32)
    longest = over_dp(jnp.full((1, 128), longest), jnp.maximum)[0, 0]
    first, send, longest = lax.optimization_barrier((first, send, longest))
    got = exchange(send)
    last = slice(3 * OWN // 4, OWN)
    got, longest = lax.optimization_barrier((got, longest))
    none = lambda v: jnp.zeros((OWN // 4, ROWS, 128), BF16)
    far = lax.cond(longest > LONG, lambda v: exchange(v)[last], none, x)
    return first, got, far


def make_rhs(first, text_lanes):
    wide = pltpu.VMEM((OWN * 152, 128), F32)
    return call(
        build_sides,
        (jax.ShapeDtypeStruct((2, KP, KP), BF16),) * NCH + (jax.ShapeDtypeStruct((8, NN), F32),) * NCH,
        2,
        (wide, wide, wide, pltpu.VMEM((NCH * NN, 128), F32)),
        mib=32,
    )(first, text_lanes)


def run_search(chunk, first_row, *operands):
    more = (pltpu.VMEM((OWN // 4, ROWS, 128), BF16), pltpu.SemaphoreType.DMA) if chunk else ()
    return call(
        functools.partial(search, chunk, first_row),
        jax.ShapeDtypeStruct((OWN, 8, 128), F32),
        len(operands),
        (
            pltpu.VMEM((MB, 2 * KP), BF16),
            pltpu.VMEM((FR // 8, 8, NN), F32),
            pltpu.VMEM((FB, NN), F32),
            pltpu.VMEM((FB, NN), F32),
            *more,
        ),
        smem=(0,),
        hbm=(7,) if chunk else (),
    )(*operands)


def pack_call(body, rows, *operands):
    return call(
        body,
        jax.ShapeDtypeStruct((OWN, rows, 128), BF16),
        len(operands),
        (pltpu.VMEM((OWN * PAD, 128), F32),),
    )(*operands)


def ranks(frame_lens):
    ids = jnp.arange(GRP, dtype=jnp.int32)
    a, b = frame_lens[:, None], frame_lens[None, :]
    ahead = (a > b) | ((a == b) & (ids[:, None] < ids[None, :]))
    return jnp.sum(ahead.astype(jnp.int32), axis=0)[None, :]


def owned(lens, rank, own):
    slots = jnp.arange(GRP // OWN, dtype=jnp.int32) * OWN + own
    return jnp.sum(jnp.where(rank == slots[:, None], lens[None, :], 0), axis=1)


def lanes_of(lens):
    parts = jnp.repeat(lens.reshape(NCH, 1, NU), OWN, axis=2)
    return jnp.broadcast_to(parts, (NCH, 8, 128))


def counts_of(frame_own):
    longest = jnp.max(frame_own.reshape(NCH, NU), axis=1)
    return jnp.concatenate([(longest + MB - 1) // MB, (longest + 2 * FB - 1) // (2 * FB)])


def shards(means, log_scales, latents, text_lens, frame_lens):
    own = lax.axis_index(SEQ).astype(jnp.int32)
    rank = ranks(frame_lens)
    text_own, frame_own = owned(text_lens, rank, own), owned(frame_lens, rank, own)
    means, log_scales, latents = (jnp.transpose(x, (1, 2, 0)) for x in (means, log_scales, latents))
    packed = pack_whole(rank, means, log_scales, latents)
    packed, later_rank, latents, later_lens = lax.optimization_barrier((packed, rank, latents, frame_lens))
    first = exchange(packed)
    packed = pack_call(pack_second, ROWS, later_rank, latents)
    first, second, far = exchange_short(first, packed, later_rank, later_lens)
    text_lanes, frame_lanes, counts = lanes_of(text_own), lanes_of(frame_own), counts_of(frame_own)
    rhs0, rhs1, bias0, bias1 = make_rhs(first, text_lanes)
    back = run_search(0, 2 * PROWS, counts, first, rhs0, bias0, text_lanes, frame_lanes)
    back = exchange(run_search(1, 0, counts, second, rhs1, bias1, text_lanes, frame_lanes, back, far))
    sums = over_dp(sum_up(back, frame_lens), jnp.add)
    pos = call(
        unpack, jax.ShapeDtypeStruct((FB, GRP), F32), 2, (pltpu.VMEM((128, 2 * 128), F32),)
    )(rank, back.reshape(OWN * 8, 128))
    return (jnp.transpose(pos), -sums[0, 64] / sums[0, 0])


def solution(mesh):
    torus = Mesh(mesh.devices.reshape(4, 2, 4, 8), ("dp_0", "dp_1", "seq_0", "seq_1"))
    in_specs = (P(DP, SEQ, None), P(DP, SEQ, None), P(DP, SEQ, None), P(DP), P(DP))
    out_specs = (P(DP, SEQ), P())
    return jax.shard_map(
        shards, mesh=torus, in_specs=in_specs, out_specs=out_specs, check_vma=False
    )
```
